32 devices in a mesh: seq: 8 (over y, x, core), dp: 4 (over z).
Axes of the slice: x: 2, y: 2, z: 4, core: 2. Of those that a mesh axis runs over, the one named last changes fastest.
Arguments:
- queries: bfloat16 [8, 512, 4096], P('dp', 'seq'), may hold values from -8 to 8
- unrotated_key_rows: bfloat16 [8, 512, 1024], P('dp', 'seq'), may hold values from -8 to 8
- value_projection_rows: bfloat16 [8, 512, 1024], P('dp', 'seq'), may hold values from -6 to 6
- attention_output_gradient: bfloat16 [8, 512, 4096], P('dp', 'seq'), may hold values from -16 to 16
- normed_hidden_input: bfloat16 [8, 512, 4096], P('dp', 'seq'), may hold values from -6 to 6
- adapter_down_weight: bfloat16 [4096, 64], replicated, may hold values from -0.01171875 to 0.01171875
- adapter_up_weight: bfloat16 [64, 4096], replicated, may hold values from -0.01171875 to 0.01171875
- lengths: int32 [8], P('dp'), may hold values from 256 to 512, as said below
- offsets: int32 [8], P('dp'), may hold values from 0 to 31
Outputs:
- grad_query: bfloat16 [8, 512, 4096], P('dp', 'seq')
- grad_key: bfloat16 [8, 512, 1024], P('dp', 'seq')
- grad_value: bfloat16 [8, 512, 1024], P('dp', 'seq')
- grad_down: float32 [4096, 64], P('seq')
- grad_up: float32 [64, 4096], P(None, 'seq')
The draws below stay inside these ranges and needn't reach their ends.
Inputs may be any that keep to these rules, and one draw needn't show every extreme that they name: `lengths`: in every draw at least one rollout has all 512 positions valid.
All inputs are finite; a program needn't handle non-finite values.
Results may differ from the reference program's by a relative error of at most 0.018.
The reference program's roundings to bfloat16 on the way count: a program that leaves them out, or rounds other values in their place, can miss the bound.
Values may be sent and summed in bfloat16 or wider, within the bound.
A program may use at most 64 MiB of HBM per device.

```python
import jax
import jax.numpy as jnp
from jax import lax

MODEL_WIDTH = 4096
QUERY_HEADS = 32
KVH = 8
HEAD_WIDTH = 128
ADAPTER_RANK = 64
TOK_DEV = 64
SEQ_LEN = 512
ROLLOUTS = 8


def draw_queries(key, part):
    drawn = jnp.clip(jax.random.normal(jax.random.fold_in(key, 1), (ROLLOUTS, SEQ_LEN, QUERY_HEADS, HEAD_WIDTH), jnp.float32), -8.0, 8.0)
    return drawn.reshape(ROLLOUTS, SEQ_LEN, QUERY_HEADS * HEAD_WIDTH).astype(jnp.bfloat16)


def draw_unrotated_key_rows(key, part):
    drawn = jnp.clip(jax.random.normal(jax.random.fold_in(key, 2), (ROLLOUTS, SEQ_LEN, KVH, HEAD_WIDTH), jnp.float32), -8.0, 8.0)
    return drawn.reshape(ROLLOUTS, SEQ_LEN, KVH * HEAD_WIDTH).astype(jnp.bfloat16)


def draw_lengths(key, part):
    picks = jax.random.randint(jax.random.fold_in(key, 21), (ROLLOUTS,), SEQ_LEN // 2, SEQ_LEN + 1)
    longest = jax.random.randint(jax.random.fold_in(key, 22), (), 0, ROLLOUTS)
    return jnp.where(jnp.arange(ROLLOUTS, dtype=jnp.int32) == longest, SEQ_LEN, picks).astype(jnp.int32)


def with_ends(values, stream_key, least, high):
    extent = values.shape
    spot = [jax.random.randint(jax.random.fold_in(stream_key, axis), (), 0, extent[axis]) for axis in range(len(extent))]
    values = values.at[tuple(spot)].set(least)
    longest = extent.index(max(extent))
    spot[longest] = (spot[longest] + 1) % extent[longest]
    return values.at[tuple(spot)].set(high)


def level_of(key, dims, cuts, least, top_value):
    level, own = 1.0, jax.random.fold_in(key, 6)
    for dim, parts in cuts:
        draws = jnp.exp(jax.random.uniform(jax.random.fold_in(own, dim), (parts,), jnp.float32, least / len(cuts), top_value / len(cuts)))
        level = level * jnp.repeat(draws, dims[dim] // parts).reshape([-1 if axis == dim else 1 for axis in range(len(dims))])
    return level


def noise(key, extent, spread, reach, pieces=(), held_as=jnp.bfloat16):
    values = jax.random.normal(key, extent, jnp.float32) * spread
    if len(pieces) > 0:
        values = level_of(key, extent, pieces, -0.22, 0.18) * values
    return jnp.clip(values, min=-reach, max=reach).astype(held_as)


def setup_inputs(seed: int = 0) -> dict:
    seeds = jax.random.split(jax.random.key(seed), 10)
    queries = draw_queries(jax.random.fold_in(seeds[9], 71), 0)
    unrotated_key_rows = draw_unrotated_key_rows(jax.random.fold_in(seeds[9], 71), 0)
    value_projection_rows = noise(seeds[2], (ROLLOUTS, SEQ_LEN, KVH * HEAD_WIDTH), 1.0, 6.0, ((0, 4), (1, 8)))
    attention_output_gradient = noise(seeds[3], (ROLLOUTS, SEQ_LEN, QUERY_HEADS * HEAD_WIDTH), 4.0, 16.0, ((0, 4), (1, 8)))
    normed_hidden_input = noise(seeds[4], (ROLLOUTS, SEQ_LEN, MODEL_WIDTH), 1.0, 6.0, ((0, 4), (1, 8)))
    adapter_down_weight = noise(seeds[5], (MODEL_WIDTH, ADAPTER_RANK), (MODEL_WIDTH * 64) ** -0.5, 0.01171875)
    adapter_up_weight = noise(seeds[6], (ADAPTER_RANK, QUERY_HEADS * HEAD_WIDTH), (QUERY_HEADS * HEAD_WIDTH * 64) ** -0.5, 0.01171875)
    lengths = draw_lengths(jax.random.fold_in(seeds[9], 71), 0)
    offsets = with_ends(jax.random.randint(seeds[8], (ROLLOUTS,), 0, TOK_DEV // 2), jax.random.fold_in(seeds[8], 1), 0, (TOK_DEV // 2) - 1).astype(jnp.int32)
    return {"queries": queries, "unrotated_key_rows": unrotated_key_rows, "value_projection_rows": value_projection_rows, "attention_output_gradient": attention_output_gradient, "normed_hidden_input": normed_hidden_input, "adapter_down_weight": adapter_down_weight, "adapter_up_weight": adapter_up_weight, "lengths": lengths, "offsets": offsets}


rotary_base = 500000.0


def rotary_tables(length, head_size):
    half_size = head_size // 2
    frequency = rotary_base ** (-(jnp.arange(half_size, dtype=jnp.float32) * 2.0 / head_size))
    angles = jnp.arange(length, dtype=jnp.float32)[:, None] * frequency[None, :]
    return jnp.cos(angles), jnp.sin(angles)


def rotate(fields, cosine, sine_table, direction):
    half_size = fields.shape[-1] // 2
    first_half = fields[..., :half_size]
    second_half = fields[..., half_size:]
    cos_wide = cosine[:, None, :]
    sin_wide = direction * sine_table[:, None, :]
    return jnp.concatenate([first_half * cos_wide - second_half * sin_wide, second_half * cos_wide + first_half * sin_wide], axis=-1)


def head_backward(rot_query, rot_key, value_head, grad_head, offset, block_rows):
    length = rot_query.shape[0]
    head_size = rot_query.shape[1]
    score_scale = head_size ** -0.5
    key_accum = jnp.zeros((length, head_size), jnp.float32)
    value_accum = jnp.zeros((length, head_size), jnp.float32)
    query_parts = []
    for block_index in range(length // block_rows):
        begin_row = block_index * block_rows
        end_row = begin_row + block_rows
        row_index = jnp.arange(begin_row, end_row, dtype=jnp.int32)[:, None]
        col_index = jnp.arange(end_row, dtype=jnp.int32)[None, :]
        visible = (col_index == row_index) | ((col_index >= offset) & (col_index <= row_index))
        query_block = rot_query[begin_row:end_row]
        grad_block = grad_head[begin_row:end_row]
        key_block = rot_key[:end_row]
        value_block = value_head[:end_row]
        scores = jnp.dot(query_block, key_block.T, preferred_element_type=jnp.float32) * score_scale
        row_max = jnp.max(jnp.where(visible, scores, -jnp.inf), axis=1, keepdims=True)
        weights_exp = jnp.where(visible, jnp.exp(scores - row_max), 0.0)
        probability = weights_exp / jnp.sum(weights_exp, axis=1, keepdims=True)
        prob_low = probability.astype(jnp.bfloat16)
        grad_prob = jnp.dot(grad_block, value_block.T, preferred_element_type=jnp.float32)
        row_delta = jnp.sum(probability * grad_prob, axis=1, keepdims=True)
        grad_score = (probability * (grad_prob - row_delta) * score_scale).astype(jnp.bfloat16)
        query_parts.append(jnp.dot(grad_score, key_block, preferred_element_type=jnp.float32))
        key_accum = key_accum.at[:end_row].add(jnp.dot(grad_score.T, query_block, preferred_element_type=jnp.float32))
        value_accum = value_accum.at[:end_row].add(jnp.dot(prob_low.T, grad_block, preferred_element_type=jnp.float32))
    return jnp.concatenate(query_parts, axis=0), key_accum, value_accum


def take_head(source, chosen_head):
    return lax.dynamic_index_in_dim(source, chosen_head, 1, keepdims=False)


def reference(queries, unrotated_key_rows, value_projection_rows, attention_output_gradient, normed_hidden_input, adapter_down_weight, adapter_up_weight, lengths, offsets):
    length = queries.shape[1]
    query_width = queries.shape[2]
    head_count = query_width // HEAD_WIDTH
    key_groups = unrotated_key_rows.shape[2] // HEAD_WIDTH
    group_size = head_count // key_groups
    block_rows = min(512, length)
    cosine, sine_table = rotary_tables(length, HEAD_WIDTH)
    positions = jnp.arange(length, dtype=jnp.int32)

    def one_rollout(inputs):
        query_sequence, key_sequence, value_sequence, grad_sequence, valid_length, offset = inputs
        keep_mask = (positions >= offset) & (positions < valid_length)
        grad_sequence = jnp.where(keep_mask[:, None], grad_sequence, jnp.zeros_like(grad_sequence))
        rot_query = rotate(query_sequence.reshape(length, head_count, HEAD_WIDTH).astype(jnp.float32), cosine, sine_table, 1.0).astype(jnp.bfloat16)
        rot_key = rotate(key_sequence.reshape(length, key_groups, HEAD_WIDTH).astype(jnp.float32), cosine, sine_table, 1.0).astype(jnp.bfloat16)
        value_heads = value_sequence.reshape(length, key_groups, HEAD_WIDTH)
        grad_heads = grad_sequence.reshape(length, head_count, HEAD_WIDTH)

        def one_head(head_index):
            key_index = head_index // group_size
            query_grad, key_grad, value_grad = head_backward(take_head(rot_query, head_index), take_head(rot_key, key_index), take_head(value_heads, key_index), take_head(grad_heads, head_index), offset, block_rows)
            query_grad = rotate(query_grad[:, None, :], cosine, sine_table, -1.0)[:, 0].astype(jnp.bfloat16)
            key_grad = rotate(key_grad[:, None, :], cosine, sine_table, -1.0)[:, 0].astype(jnp.bfloat16)
            return query_grad, key_grad, value_grad.astype(jnp.bfloat16)

        query_all, key_all, value_all = lax.map(one_head, jnp.arange(head_count, dtype=jnp.int32))
        rollout_query = jnp.transpose(query_all, (1, 0, 2)).reshape(length, query_width)
        key_sum = key_all.astype(jnp.float32).reshape(key_groups, group_size, length, HEAD_WIDTH).sum(axis=1).astype(jnp.bfloat16)
        value_sum = value_all.astype(jnp.float32).reshape(key_groups, group_size, length, HEAD_WIDTH).sum(axis=1).astype(jnp.bfloat16)
        rollout_key = jnp.transpose(key_sum, (1, 0, 2)).reshape(length, key_groups * HEAD_WIDTH)
        rollout_value = jnp.transpose(value_sum, (1, 0, 2)).reshape(length, key_groups * HEAD_WIDTH)
        return rollout_query, rollout_key, rollout_value

    grad_query, grad_key, grad_value = lax.map(one_rollout, (queries, unrotated_key_rows, value_projection_rows, attention_output_gradient, lengths, offsets))
    hidden_state = normed_hidden_input.reshape(-1, normed_hidden_input.shape[2])
    flattened_query = grad_query.reshape(-1, query_width)
    adapter_latent = jnp.dot(hidden_state, adapter_down_weight, preferred_element_type=jnp.float32).astype(jnp.bfloat16)
    backward_gradient = jnp.dot(flattened_query, adapter_up_weight.T, preferred_element_type=jnp.float32).astype(jnp.bfloat16)
    grad_down = jnp.dot(hidden_state.T, backward_gradient, preferred_element_type=jnp.float32)
    grad_up = jnp.dot(adapter_latent.T, flattened_query, preferred_element_type=jnp.float32)
    return grad_query, grad_key, grad_value, grad_down, grad_up
```

```python
from functools import partial

import math

import jax
import jax.numpy as jnp
import numpy as np
from jax import lax
from jax.experimental import pallas as pl
from jax.experimental.pallas import tpu as pltpu
from jax.sharding import PartitionSpec as P

HEAD_WIDTH = 128


rotary_base = 500000.0


def partner_2(value, axis, distance):
    mask = 2**distance
    pairs = [(source, source ^ mask) for source in range(lax.axis_size(axis))]
    return lax.ppermute(value, axis, pairs)


def rotary_tables(length, head_size):
    half_size = head_size // 2
    frequency = rotary_base ** (-(jnp.arange(half_size, dtype=jnp.float32) * 2.0 / head_size))
    angles = jnp.arange(length, dtype=jnp.float32)[:, None] * frequency[None, :]
    return (jnp.cos(angles), jnp.sin(angles))


def rotate(fields, cosine, sine_table, direction):
    half_size = fields.shape[-1] // 2
    first_half = fields[..., :half_size]
    second_half = fields[..., half_size:]
    cos_wide = cosine[:, None, :]
    sin_wide = direction * sine_table[:, None, :]
    return jnp.concatenate(
        [
            first_half * cos_wide - second_half * sin_wide,
            second_half * cos_wide + first_half * sin_wide,
        ],
        axis=-1,
    )


def contract_axes(first_operand, second_operand, first_axis, second_axis):
    return lax.dot_general(
        first_operand,
        second_operand,
        (((first_axis,), (second_axis,)), ((), ())),
        preferred_element_type=jnp.float32,
    )


def block_terms(rot_query, rot_key, value_head, grad_head, offset, begin_row, end_row, score_scale):
    row_index = jnp.arange(begin_row, end_row, dtype=jnp.int32)[:, None]
    col_index = jnp.arange(end_row, dtype=jnp.int32)[None, :]
    visible = (col_index == row_index) | (col_index >= offset) & (col_index <= row_index)
    query_block = rot_query[begin_row:end_row]
    grad_block = grad_head[begin_row:end_row]
    key_block = rot_key[:end_row]
    value_block = value_head[:end_row]
    scores = contract_axes(query_block, key_block, 1, 1) * score_scale
    row_max = jnp.max(jnp.where(visible, scores, -jnp.inf), axis=1, keepdims=True)
    row_total = jnp.sum(jnp.where(visible, jnp.exp(scores - row_max), 0.0), axis=1, keepdims=True)
    grad_prob = contract_axes(grad_block, value_block, 1, 1)
    probability = jnp.where(visible, jnp.exp(scores - row_max), 0.0) / row_total
    row_delta = jnp.sum(probability * grad_prob, axis=1, keepdims=True)
    prob_low = probability.astype(jnp.bfloat16)
    grad_score = (probability * (grad_prob - row_delta) * score_scale).astype(jnp.bfloat16)
    block_grad = jnp.dot(grad_score, key_block, preferred_element_type=jnp.float32)
    key_add = contract_axes(grad_score, query_block, 0, 0)
    value_add = contract_axes(prob_low, grad_block, 0, 0)
    return (block_grad, key_add, value_add)


def head_backward(rot_query, rot_key, value_head, grad_head, offset, block_rows):
    length = rot_query.shape[0]
    head_size = rot_query.shape[1]
    score_scale = head_size ** (-0.5)
    query_parts = []
    key_terms = []
    value_terms = []
    for block_index in range(length // block_rows):
        begin_row = block_index * block_rows
        end_row = begin_row + block_rows
        live_terms = partial(
            block_terms,
            rot_query,
            rot_key,
            value_head,
            grad_head,
            offset,
            begin_row,
            end_row,
            score_scale,
        )
        results = live_terms()
        block_grad, key_add, value_add = results
        query_parts.append(block_grad)
        key_terms.append(jnp.pad(key_add, ((0, length - end_row), (0, 0))))
        value_terms.append(jnp.pad(value_add, ((0, length - end_row), (0, 0))))
    key_accum = key_terms[0]
    value_accum = value_terms[0]
    for term_index in range(1, len(key_terms)):
        key_accum = key_accum + key_terms[term_index]
        value_accum = value_accum + value_terms[term_index]
    return (jnp.concatenate(query_parts, axis=0), key_accum, value_accum)


def arrange_rows(rows, share, part_rows, key_groups):
    rollout_count = rows.shape[0]
    split = rows.reshape(rollout_count, share, part_rows, key_groups, HEAD_WIDTH)
    return jnp.transpose(split, (0, 2, 3, 1, 4)).reshape(
        rollout_count, part_rows, key_groups * share, HEAD_WIDTH
    )


def join_group(paired, share, seq_parts, part_rows):
    my_index = lax.axis_index("seq")
    rollout_count = paired.shape[1]
    local_keys = paired.shape[3]
    joined = paired[None]
    for bit in range(share.bit_length() - 1):
        partner = partner_2(joined, "seq", bit)
        upper = my_index // (1 << bit) % 2
        joined = jnp.where(
            upper == 0,
            jnp.concatenate([joined, partner], axis=0),
            jnp.concatenate([partner, joined], axis=0),
        )
    ordered = joined.reshape(share, 2, rollout_count, seq_parts, part_rows, local_keys, HEAD_WIDTH)
    ordered = jnp.transpose(ordered, (1, 2, 3, 0, 4, 5, 6))
    return ordered.reshape(2, rollout_count, seq_parts * share * part_rows, local_keys, HEAD_WIDTH)


def reduce_group(partial_sums, share, seq_parts, part_rows):
    my_index = lax.axis_index("seq")
    rollout_count = partial_sums.shape[1]
    local_keys = partial_sums.shape[3]
    split = partial_sums.reshape(
        2, rollout_count, seq_parts, share, part_rows, local_keys, HEAD_WIDTH
    )
    split = jnp.transpose(split, (3, 0, 1, 2, 4, 5, 6))
    for bit in reversed(range(share.bit_length() - 1)):
        half = split.shape[0] // 2
        lower_half = split[:half]
        upper_half = split[half:]
        upper = my_index // (1 << bit) % 2
        keep = jnp.where(upper == 0, lower_half, upper_half)
        outgoing = jnp.where(upper == 0, upper_half, lower_half)
        split = keep + partner_2(outgoing.astype(jnp.bfloat16), "seq", bit).astype(outgoing.dtype)
    return split[0].reshape(2, rollout_count, seq_parts * part_rows, local_keys, HEAD_WIDTH)


def on_device(
    queries,
    unrotated_key_rows,
    value_projection_rows,
    attention_output_gradient,
    normed_hidden_input,
    adapter_down_weight,
    adapter_up_weight,
    lengths,
    offsets,
):
    rollout_count = queries.shape[0]
    tokens = queries.shape[1]
    seq_parts = lax.axis_size("seq")
    length = tokens * seq_parts
    query_width = queries.shape[2]
    head_count = query_width // HEAD_WIDTH
    key_groups = unrotated_key_rows.shape[2] // HEAD_WIDTH
    local_heads = head_count // seq_parts
    adapter_rank_size = adapter_down_weight.shape[1]
    share = max(1, seq_parts // key_groups)
    part_rows = tokens // share
    query_tokens = queries.reshape(rollout_count, tokens, head_count, HEAD_WIDTH)
    grad_tokens = attention_output_gradient.reshape(rollout_count, tokens, head_count, HEAD_WIDTH)
    key_arranged = arrange_rows(unrotated_key_rows, share, part_rows, key_groups)
    value_arranged = arrange_rows(value_projection_rows, share, part_rows, key_groups)
    query_heads, key_parted, value_parted, grad_heads = (
        lax.all_to_all(query_tokens, "seq", split_axis=2, concat_axis=1, tiled=True),
        lax.all_to_all(key_arranged, "seq", split_axis=2, concat_axis=1, tiled=True),
        lax.all_to_all(value_arranged, "seq", split_axis=2, concat_axis=1, tiled=True),
        lax.all_to_all(grad_tokens, "seq", split_axis=2, concat_axis=1, tiled=True),
    )
    paired = join_group(jnp.stack([key_parted, value_parted], axis=0), share, seq_parts, part_rows)
    key_heads = paired[0]
    value_heads = paired[1]
    local_keys = key_heads.shape[2]
    cosine, sine_table = rotary_tables(length, HEAD_WIDTH)
    positions = jnp.arange(length, dtype=jnp.int32)
    keep_mask = (positions[None, :] >= offsets[:, None]) & (positions[None, :] < lengths[:, None])
    grad_heads = jnp.where(keep_mask[:, :, None, None], grad_heads, jnp.zeros_like(grad_heads))
    rot_query = rotate(query_heads.astype(jnp.float32), cosine, sine_table, 1.0).astype(
        jnp.bfloat16
    )
    rot_key = rotate(key_heads.astype(jnp.float32), cosine, sine_table, 1.0).astype(jnp.bfloat16)
    block_rows = min(512, length)
    query_rolls = []
    key_rolls = []
    value_rolls = []
    for rollout_slot in range(rollout_count):
        query_list = []
        key_list = []
        value_list = []
        for head_slot in range(local_heads):
            key_slot = head_slot * local_keys // local_heads
            query_grad, key_grad, value_grad = head_backward(
                rot_query[rollout_slot, :, head_slot],
                rot_key[rollout_slot, :, key_slot],
                value_heads[rollout_slot, :, key_slot],
                grad_heads[rollout_slot, :, head_slot],
                offsets[rollout_slot],
                block_rows,
            )
            query_list.append(
                rotate(query_grad[:, None, :], cosine, sine_table, -1.0)[:, 0].astype(jnp.bfloat16)
            )
            key_list.append(
                rotate(key_grad[:, None, :], cosine, sine_table, -1.0)[:, 0].astype(jnp.bfloat16)
            )
            value_list.append(value_grad.astype(jnp.bfloat16))
        query_rolls.append(jnp.stack(query_list, axis=1))
        key_rolls.append(jnp.stack(key_list, axis=1))
        value_rolls.append(jnp.stack(value_list, axis=1))
    query_back = jnp.stack(query_rolls, axis=0)
    key_parts = jnp.stack(key_rolls, axis=0)
    value_parts = jnp.stack(value_rolls, axis=0)
    shared_heads = local_heads // local_keys
    key_local = (
        key_parts.astype(jnp.float32)
        .reshape(rollout_count, length, local_keys, shared_heads, HEAD_WIDTH)
        .sum(axis=3)
    )
    value_local = (
        value_parts.astype(jnp.float32)
        .reshape(rollout_count, length, local_keys, shared_heads, HEAD_WIDTH)
        .sum(axis=3)
    )
    summed = reduce_group(
        jnp.stack([key_local, value_local], axis=0), share, seq_parts, part_rows
    ).astype(jnp.bfloat16)
    query_result, key_result, value_result = (
        lax.all_to_all(query_back, "seq", split_axis=1, concat_axis=2, tiled=True),
        lax.all_to_all(summed[0], "seq", split_axis=1, concat_axis=2, tiled=True),
        lax.all_to_all(summed[1], "seq", split_axis=1, concat_axis=2, tiled=True),
    )
    key_total = jnp.transpose(
        key_result.reshape(rollout_count, part_rows, key_groups, share, HEAD_WIDTH), (0, 3, 1, 2, 4)
    ).reshape(rollout_count, tokens, key_groups * HEAD_WIDTH)
    value_total = jnp.transpose(
        value_result.reshape(rollout_count, part_rows, key_groups, share, HEAD_WIDTH),
        (0, 3, 1, 2, 4),
    ).reshape(rollout_count, tokens, key_groups * HEAD_WIDTH)
    flattened_query = query_result.reshape(rollout_count * tokens, query_width)
    hidden_state = normed_hidden_input.reshape(rollout_count * tokens, normed_hidden_input.shape[2])
    adapter_latent = jnp.dot(
        hidden_state, adapter_down_weight, preferred_element_type=jnp.float32
    ).astype(jnp.bfloat16)
    backward_gradient = contract_axes(flattened_query, adapter_up_weight, 1, 1).astype(jnp.bfloat16)
    joined_terms = lax.psum_scatter(
        jnp.concatenate(
            [
                contract_axes(hidden_state, backward_gradient, 0, 0),
                contract_axes(flattened_query, adapter_latent, 0, 0),
            ],
            axis=1,
        ).astype(jnp.bfloat16),
        "seq",
        scatter_dimension=0,
        tiled=True,
    ).astype(jnp.float32)
    down_local = joined_terms[:, :adapter_rank_size]
    up_local = joined_terms[:, adapter_rank_size:]
    down_sum, up_sum = (
        lax.psum(down_local.astype(jnp.bfloat16), "dp").astype(jnp.float32),
        lax.psum(up_local.astype(jnp.bfloat16), "dp").astype(jnp.float32),
    )
    return (
        flattened_query.reshape(rollout_count, tokens, query_width),
        key_total,
        value_total,
        down_sum,
        up_sum.T,
    )


VMEM_LIMIT = 48 * 1024 * 1024
NEG = -1e30
OFFSET_BOUND = 32


def nt_dot(left, right):
    return lax.dot_general(
        left, right, (((1,), (1,)), ((), ())), preferred_element_type=jnp.float32
    )


def fused_kernel(
    n_seq,
    n_dp,
    n_roll,
    tokens,
    kv_heads,
    group,
    rank,
    off_hbm,
    len_hbm,
    cos_hbm,
    sin_hbm,
    q_hbm,
    k_hbm,
    v_hbm,
    g_hbm,
    hid_hbm,
    down_hbm,
    up_hbm,
    gq_ref,
    gk_ref,
    gv_ref,
    gd_ref,
    gu_ref,
    off_ref,
    len_ref,
    cos_ref,
    sin_ref,
    k_raw,
    kv_own,
    kv_all,
    q_all,
    g_all,
    hid_own,
    hid_other,
    down_ref,
    up_ref,
    lat_all,
    lat_roll,
    score_buf,
    prob_buf,
    dkv_own,
    dkv_all,
    gq_all,
    back_acc,
    back_got,
    up_acc,
    up_own,
    up_got,
    dn_own,
    dn_got,
    z_own,
    z_got,
    z_all,
    loc_sem,
    v_sem,
    ql_sem,
    gl_sem,
    kv_send,
    kv_recv,
    q_send,
    q_recv,
    g_send,
    g_recv,
    hid_send,
    hid_recv,
    one_send,
    one_recv,
    dk_send,
    dk_recv,
    gq_send,
    gq_recv,
    ad_send,
    ad_recv,
    rs_send,
    rs_recv,
    ag_send,
    ag_recv,
):
    me = lax.axis_index("seq")
    my_dp = lax.axis_index("dp")
    chip = me // 2
    core = me % 2
    partner = me + 1 - 2 * core
    n_chips = n_seq // 2
    n_own = kv_heads // 2
    width = HEAD_WIDTH
    half = width // 2
    span = group * width
    chip_tokens = 2 * tokens
    rows = group * chip_tokens
    scale = width ** (-0.5)
    exp_scale = scale * math.log2(math.e)
    piece = span // n_dp

    def lanes(index, size):
        return pl.ds(pl.multiple_of(index * size, size), size)

    def seq_rows(device):
        return pl.ds(pl.multiple_of(device * tokens, tokens), tokens)

    def local(src, dst, sem):
        return pltpu.make_async_copy(src, dst, sem)

    def remote(src, dst, send, recv, where):
        return pltpu.make_async_remote_copy(
            src_ref=src, dst_ref=dst, send_sem=send, recv_sem=recv, device_id=where
        )

    def each_unit(body):
        def step(index, carry):
            body(index // n_roll, index % n_roll)
            return carry

        lax.fori_loop(0, n_own * n_roll, step, 0)

    barrier = pltpu.get_barrier_semaphore()
    for step in range(1, n_seq):
        pl.semaphore_signal(barrier, inc=1, device_id={"seq": lax.rem(me + step, n_seq)})
    for step in range(1, n_dp):
        pl.semaphore_signal(barrier, inc=1, device_id={"dp": lax.rem(my_dp + step, n_dp)})

    chip_rows = pl.ds(pl.multiple_of(chip * chip_tokens, chip_tokens), chip_tokens)
    k_load = local(k_hbm, k_raw, loc_sem.at[0])
    cos_load = local(cos_hbm.at[chip_rows], cos_ref, loc_sem.at[1])
    sin_load = local(sin_hbm.at[chip_rows], sin_ref, loc_sem.at[2])
    off_load = local(off_hbm, off_ref, loc_sem.at[3])
    len_load = local(len_hbm, len_ref, loc_sem.at[4])
    hid_load = local(hid_hbm, hid_own, loc_sem.at[5])
    down_load = local(down_hbm, down_ref, loc_sem.at[6])
    up_load = local(up_hbm, up_ref, loc_sem.at[7])

    def v_load(h):
        return local(v_hbm.at[:, :, lanes(h, width)], kv_own.at[h, :, 1], v_sem.at[h])

    def q_load(i, r):
        h = 2 * i + core
        return local(q_hbm.at[r, :, lanes(h, span)], q_all.at[i, r, core], ql_sem.at[i, r])

    def g_load(i, r):
        h = 2 * i + core
        return local(g_hbm.at[r, :, lanes(h, span)], g_all.at[i, r, core], gl_sem.at[i, r])

    def load_queries(i, r):
        q_load(i, r).start()
        g_load(i, r).start()

    k_load.start()
    cos_load.start()
    sin_load.start()
    for h in range(kv_heads):
        v_load(h).start()
    off_load.start()
    len_load.start()
    each_unit(load_queries)
    hid_load.start()
    down_load.start()
    up_load.start()

    def q_copy(i, r):
        h = 2 * i + 1 - core
        return remote(
            q_hbm.at[r, :, lanes(h, span)],
            q_all.at[i, r, core],
            q_send.at[i, r],
            q_recv.at[i, r],
            {"seq": partner},
        )

    def g_copy(i, r):
        h = 2 * i + 1 - core
        return remote(
            g_hbm.at[r, :, lanes(h, span)],
            g_all.at[i, r, core],
            g_send.at[i, r],
            g_recv.at[i, r],
            {"seq": partner},
        )

    def hid_copy(i):
        h = 2 * i + 1 - core
        return remote(
            hid_hbm.at[:, :, lanes(h, span)],
            hid_other.at[i],
            hid_send.at[i],
            hid_recv.at[i],
            {"seq": partner},
        )

    def send_queries(i, r):
        q_copy(i, r).start()
        g_copy(i, r).start()

    def gather_copy(i, r, parity, chip_step):
        h = 2 * i + parity
        return remote(
            kv_own.at[h, r],
            kv_all.at[i, r, :, seq_rows(me), :],
            kv_send.at[i, r, parity, chip_step],
            kv_recv.at[i, r, me],
            {"seq": 2 * (chip + chip_step) + parity},
        )

    def pair_copy(i, r):
        h = 2 * i + 1 - core
        return remote(
            kv_own.at[h, r],
            kv_all.at[i, r, :, seq_rows(me), :],
            kv_send.at[i, r, 0, 0],
            kv_recv.at[i, r, me],
            {"seq": partner},
        )

    def gather_ops(i, r, act):
        act(pair_copy(i, r))
        for chip_step in range(1, n_chips):

            @pl.when(chip + chip_step < n_chips)
            def _():
                for parity in range(2):
                    act(gather_copy(i, r, parity, chip_step))

    def gather_wait(i, r):
        def got(device):
            remote(
                kv_own.at[0, r],
                kv_all.at[i, r, :, seq_rows(device), :],
                kv_send.at[i, r, 0, 0],
                kv_recv.at[i, r, device],
                {"seq": partner},
            ).wait_recv()

        got(partner)
        for source in range(n_chips - 1):

            @pl.when(source < chip)
            def _():
                got(2 * source)
                got(2 * source + 1)

    def reduce_copy(i, r, target_chip, target_core):
        target = 2 * target_chip + target_core
        return remote(
            dkv_own.at[i, r, :, seq_rows(target), :],
            dkv_all.at[chip, 2 * i + core, r],
            dk_send.at[i, r, target_chip, target_core],
            dk_recv.at[chip, 2 * i + core, r],
            {"seq": target},
        )

    def reduce_ops(i, r, act):
        for target_chip in range(n_chips - 1):

            @pl.when(target_chip < chip)
            def _():
                for target_core in range(2):
                    act(reduce_copy(i, r, target_chip, target_core))

        act(reduce_copy(i, r, chip, 1 - core))

    def reduce_got(source, h, r):
        return remote(
            dkv_own.at[0, 0, :, pl.ds(0, tokens), :],
            dkv_all.at[source, h, r],
            dk_send.at[0, 0, 0, 0],
            dk_recv.at[source, h, r],
            {"seq": partner},
        )

    def gq_copy(i, r, parity):
        return remote(
            gq_all.at[i, r, 1 - core],
            gq_ref.at[r, :, lanes(2 * i + parity, span)],
            gq_send.at[i, r],
            gq_recv.at[i, r],
            {"seq": partner},
        )

    def adapter_copy(t, own, got, source, target_chip):
        return remote(
            own.at[target_chip],
            got.at[source],
            ad_send.at[t, target_chip],
            ad_recv.at[t, source],
            {"seq": 2 * target_chip + core},
        )

    pl.semaphore_wait(barrier, n_seq + n_dp - 2)

    k_load.wait()
    cos_load.wait()
    sin_load.wait()
    own_rows = pl.ds(pl.multiple_of(core * tokens, tokens), tokens)
    cos_own = cos_ref[own_rows, :]
    sin_own = sin_ref[own_rows, :]
    for h in range(kv_heads):
        for r in range(n_roll):
            key = k_raw[r, :, h * width : (h + 1) * width].astype(jnp.float32)
            key = key * cos_own + pltpu.roll(key, half, 1) * sin_own
            kv_own[h, r, 0] = key.astype(jnp.bfloat16)
    for h in range(kv_heads):
        v_load(h).wait()
    each_unit(lambda i, r: gather_ops(i, r, lambda copy: copy.start()))
    each_unit(send_queries)

    for i in range(n_own):
        for r in range(n_roll):
            kv_all[i, r, :, seq_rows(me), :] = kv_own[2 * i + core, r]

    hid_load.wait()
    down_load.wait()
    flat = n_roll * tokens
    hid_rows = hid_own[...].reshape(flat, hid_own.shape[2])
    lat_all[core] = nt_dot(down_ref[...], hid_rows).astype(jnp.bfloat16)
    lat_copy = remote(
        lat_all.at[core], lat_all.at[core], one_send.at[0], one_recv.at[0], {"seq": partner}
    )
    lat_copy.start()
    for i in range(n_own):
        hid_copy(i).start()
    back_acc[...] = jnp.zeros_like(back_acc)
    up_acc[...] = jnp.zeros_like(up_acc)
    up_load.wait()
    off_load.wait()
    len_load.wait()
    remote(
        lat_all.at[core], lat_all.at[1 - core], one_send.at[0], one_recv.at[0], {"seq": partner}
    ).wait_recv()
    for r in range(n_roll):
        lane = slice(r * tokens, (r + 1) * tokens)
        lat_roll[r] = jnp.concatenate([lat_all[0, :, lane], lat_all[1, :, lane]], axis=1)

    def attend(i, r, blocks):
        n_keys = blocks * chip_tokens
        offset = off_ref[r]
        position = chip * chip_tokens + lax.broadcasted_iota(jnp.int32, (chip_tokens, width), 0)
        keep = (position >= offset) & (position < len_ref[r])
        cos = cos_ref[...]
        sin = sin_ref[...]
        queries = []
        grads = []
        for j in range(group):
            lane = slice(j * width, (j + 1) * width)
            query = q_all[i, r, :, :, lane].reshape(chip_tokens, width).astype(jnp.float32)
            query = query * cos + pltpu.roll(query, half, 1) * sin
            queries.append(query.astype(jnp.bfloat16))
            grad = g_all[i, r, :, :, lane].reshape(chip_tokens, width).astype(jnp.float32)
            grads.append(jnp.where(keep, grad, 0.0).astype(jnp.bfloat16))
        query = jnp.concatenate(queries, axis=0)
        grad = jnp.concatenate(grads, axis=0)
        key = kv_all[i, r, 0, :n_keys, :]

        row_max = None
        for b in range(blocks):
            keys = slice(b * chip_tokens, (b + 1) * chip_tokens)
            score = nt_dot(kv_all[i, r, 0, keys, :], query)
            if b == blocks - 1 or b * chip_tokens < OFFSET_BOUND:
                key_row = lax.broadcasted_iota(jnp.int32, (chip_tokens, rows), 0)
                visible = key_row + b * chip_tokens >= offset
                if b == blocks - 1:
                    query_row = lax.broadcasted_iota(jnp.int32, (chip_tokens, rows), 1) % chip_tokens
                    visible = (key_row == query_row) | (visible & (key_row <= query_row))
                score = jnp.where(visible, score, NEG)
            score_buf[0, keys, :] = score
            part = jnp.max(score, axis=0, keepdims=True)
            row_max = part if row_max is None else jnp.maximum(row_max, part)
        total = None
        delta = None
        for b in range(blocks):
            keys = slice(b * chip_tokens, (b + 1) * chip_tokens)
            weight = jnp.exp2((score_buf[0, keys, :] - row_max) * exp_scale)
            grad_prob = nt_dot(kv_all[i, r, 1, keys, :], grad)
            score_buf[0, keys, :] = weight
            score_buf[1, keys, :] = grad_prob
            part = jnp.sum(weight, axis=0, keepdims=True)
            total = part if total is None else total + part
            part = jnp.sum(weight * grad_prob, axis=0, keepdims=True)
            delta = part if delta is None else delta + part
        inverse = 1.0 / total
        delta = delta * inverse
        inverse_scaled = inverse * scale
        for b in range(blocks):
            keys = slice(b * chip_tokens, (b + 1) * chip_tokens)
            weight = score_buf[0, keys, :]
            prob = (weight * inverse).astype(jnp.bfloat16)
            slope = ((weight * inverse_scaled) * (score_buf[1, keys, :] - delta)).astype(jnp.bfloat16)
            prob_buf[keys, :] = slope
            dkv_own[i, r, 1, keys, :] = jnp.dot(
                prob, grad, preferred_element_type=jnp.float32
            ).astype(jnp.bfloat16)
            dkv_own[i, r, 0, keys, :] = jnp.dot(
                slope, query, preferred_element_type=jnp.float32
            ).astype(jnp.bfloat16)
        back = jnp.dot(key.T, prob_buf[:n_keys, :], preferred_element_type=jnp.float32).T
        for j in range(group):
            part = back[j * chip_tokens : (j + 1) * chip_tokens]
            part = part * cos - pltpu.roll(part, half, 1) * sin
            part = part.astype(jnp.bfloat16).reshape(2, tokens, width)
            gq_all[i, r, :, :, j * width : (j + 1) * width] = part

    def unit(i, r):
        h = 2 * i + core
        gather_wait(i, r)
        q_load(i, r).wait()
        g_load(i, r).wait()
        remote(
            q_hbm.at[r, :, lanes(h, span)],
            q_all.at[i, r, 1 - core],
            q_send.at[i, r],
            q_recv.at[i, r],
            {"seq": partner},
        ).wait_recv()
        remote(
            g_hbm.at[r, :, lanes(h, span)],
            g_all.at[i, r, 1 - core],
            g_send.at[i, r],
            g_recv.at[i, r],
            {"seq": partner},
        ).wait_recv()
        for blocks in range(1, n_chips + 1):

            @pl.when(chip == blocks - 1)
            def _():
                attend(i, r, blocks)

        reduce_ops(i, r, lambda copy: copy.start())
        gq_copy(i, r, core).start()
        dkv_all[chip, h, r] = dkv_own[i, r, :, seq_rows(me), :]
        gq_ref[r, :, lanes(h, span)] = gq_all[i, r, core]
        grad_query = gq_all[i, r].reshape(chip_tokens, span)
        back_acc[r] = back_acc[r] + nt_dot(up_ref[:, lanes(h, span)], grad_query)
        up_part = jnp.dot(lat_roll[r], grad_query, preferred_element_type=jnp.float32)
        up_total = jnp.where(r == 0, 0.0, up_acc[...]) + up_part
        up_acc[...] = up_total

        @pl.when(r == n_roll - 1)
        def _():
            up_own[i] = up_total.astype(jnp.bfloat16)

            @pl.when(i != chip)
            def _():
                adapter_copy(1, up_own, up_got, chip, i).start()

    each_unit(unit)

    back_copy = remote(back_acc, back_got, one_send.at[1], one_recv.at[1], {"seq": partner})
    back_copy.start()
    for i in range(n_own):
        hid_copy(i).wait_recv()
    back_copy.wait_recv()
    sums = [(back_acc[r] + back_got[r]).astype(jnp.bfloat16) for r in range(n_roll)]
    first = jnp.concatenate([part[:, :tokens] for part in sums], axis=1)
    second = jnp.concatenate([part[:, tokens:] for part in sums], axis=1)
    back_own = jnp.where(core == 0, first, second)
    back_other = jnp.where(core == 0, second, first)
    for i in range(n_own):
        own = hid_own[:, :, lanes(2 * i + core, span)].reshape(flat, span)
        other = hid_other[i].reshape(flat, span)
        dn_own[i] = (
            jnp.dot(back_own, own, preferred_element_type=jnp.float32)
            + jnp.dot(back_other, other, preferred_element_type=jnp.float32)
        ).astype(jnp.bfloat16)

        @pl.when(i != chip)
        def _():
            adapter_copy(0, dn_own, dn_got, chip, i).start()

    def owner_sum(t, own, got):
        total = own[chip].astype(jnp.float32)
        for step in range(1, n_chips):
            source = lax.rem(chip + step, n_chips)
            adapter_copy(t, own, got, source, 0).wait_recv()
            total = total + got[source].astype(jnp.float32)
        z_own[t] = total.astype(jnp.bfloat16)

    def scatter_copy(t, target):
        return remote(
            z_own.at[t, :, lanes(target, piece)],
            z_got.at[t, my_dp],
            rs_send.at[t, target],
            rs_recv.at[t, my_dp],
            {"dp": target},
        )

    def scatter_start(t):
        for step in range(1, n_dp):
            scatter_copy(t, lax.rem(my_dp + step, n_dp)).start()

    def collect_copy(t, target):
        return remote(
            z_all.at[t, my_dp],
            z_all.at[t, my_dp],
            ag_send.at[t, target],
            ag_recv.at[t, my_dp],
            {"dp": target},
        )

    def collect_start(t):
        total = z_own[t, :, lanes(my_dp, piece)].astype(jnp.float32)
        for step in range(1, n_dp):
            source = lax.rem(my_dp + step, n_dp)
            remote(
                z_own.at[t, :, lanes(source, piece)],
                z_got.at[t, source],
                rs_send.at[t, source],
                rs_recv.at[t, source],
                {"dp": source},
            ).wait_recv()
            total = total + z_got[t, source].astype(jnp.float32)
        z_all[t, my_dp] = total.astype(jnp.bfloat16)
        for step in range(1, n_dp):
            collect_copy(t, lax.rem(my_dp + step, n_dp)).start()

    def collect_out(t, out):
        for step in range(1, n_dp):
            source = lax.rem(my_dp + step, n_dp)
            remote(
                z_all.at[t, source],
                z_all.at[t, source],
                ag_send.at[t, source],
                ag_recv.at[t, source],
                {"dp": source},
            ).wait_recv()
        for d in range(n_dp):
            out[:, d * piece : (d + 1) * piece] = z_all[t, d].astype(jnp.float32)

    owner_sum(1, up_own, up_got)
    scatter_start(1)

    cos_own = cos_ref[own_rows, :]
    sin_own = sin_ref[own_rows, :]

    def finish(h, r):
        @pl.when(h % 2 != core)
        def _():
            reduce_got(chip, h, r).wait_recv()

        for source in range(1, n_chips):

            @pl.when(source > chip)
            def _():
                reduce_got(source, h, r).wait_recv()

        def add(source, totals):
            return tuple(
                totals[t] + dkv_all[source, h, r, t].astype(jnp.float32) for t in range(2)
            )

        first = tuple(dkv_all[chip, h, r, t].astype(jnp.float32) for t in range(2))
        key, value = lax.fori_loop(chip + 1, n_chips, add, first)
        key = key * cos_own - pltpu.roll(key, half, 1) * sin_own
        gk_ref[r, :, lanes(h, width)] = key.astype(jnp.bfloat16)
        gv_ref[r, :, lanes(h, width)] = value.astype(jnp.bfloat16)

    def finish_step(index, carry):
        finish(index // n_roll, index % n_roll)
        return carry

    lax.fori_loop(0, kv_heads * n_roll, finish_step, 0)

    collect_start(1)
    owner_sum(0, dn_own, dn_got)
    scatter_start(0)
    collect_out(1, gu_ref)
    each_unit(lambda i, r: gq_copy(i, r, 1 - core).wait_recv())
    collect_start(0)

    each_unit(lambda i, r: gather_ops(i, r, lambda copy: copy.wait_send()))
    each_unit(lambda i, r: reduce_ops(i, r, lambda copy: copy.wait_send()))

    def sent(i, r):
        q_copy(i, r).wait_send()
        g_copy(i, r).wait_send()
        gq_copy(i, r, core).wait_send()

    each_unit(sent)
    lat_copy.wait_send()
    back_copy.wait_send()
    for i in range(n_own):
        hid_copy(i).wait_send()

        @pl.when(i != chip)
        def _():
            adapter_copy(0, dn_own, dn_got, chip, i).wait_send()
            adapter_copy(1, up_own, up_got, chip, i).wait_send()

    collect_out(0, gd_ref)
    for t in range(2):
        for step in range(1, n_dp):
            target = lax.rem(my_dp + step, n_dp)
            scatter_copy(t, target).wait_send()
            collect_copy(t, target).wait_send()


def write_kernel(n_outs, *refs):
    sem = refs[2 * n_outs]
    copies = [
        pltpu.make_async_copy(refs[n], refs[n_outs + n], sem.at[n]) for n in range(n_outs)
    ]
    for copy in copies:
        copy.start()
    for copy in copies:
        copy.wait()


def fused_on_device(
    n_seq,
    n_dp,
    queries,
    unrotated_key_rows,
    value_projection_rows,
    attention_output_gradient,
    normed_hidden_input,
    adapter_down_weight,
    adapter_up_weight,
    lengths,
    offsets,
):
    n_roll, tokens, q_width = queries.shape
    kv_width = unrotated_key_rows.shape[2]
    kv_heads = kv_width // HEAD_WIDTH
    group = q_width // kv_width
    rank = adapter_down_weight.shape[1]
    length = n_seq * tokens
    n_chips = n_seq // 2
    n_own = kv_heads // 2
    half = HEAD_WIDTH // 2
    frequency = rotary_base ** (-(np.arange(half, dtype=np.float32) * 2.0 / HEAD_WIDTH))
    angles = np.arange(length, dtype=np.float32)[:, None] * frequency.astype(np.float32)[None, :]
    cosine, sine = np.cos(angles), np.sin(angles)
    cos_wide = np.concatenate([cosine, cosine], axis=1).astype(np.float32)
    sin_wide = np.concatenate([-sine, sine], axis=1).astype(np.float32)
    span = q_width // n_seq
    low = jnp.bfloat16
    full = jnp.float32
    dma = pltpu.SemaphoreType.DMA
    vm = pltpu.VMEM
    anywhere = pl.BlockSpec(memory_space=pl.ANY)
    vmem = pl.BlockSpec(memory_space=pltpu.VMEM)
    out_types = [
        ((n_roll, tokens, q_width), low),
        ((n_roll, tokens, kv_width), low),
        ((n_roll, tokens, kv_width), low),
        ((rank, span), full),
        ((rank, span), full),
    ]
    outs = pl.pallas_call(
        partial(fused_kernel, n_seq, n_dp, n_roll, tokens, kv_heads, group, rank),
        out_shape=[vm(shape, kind) for shape, kind in out_types],
        in_specs=[anywhere] * 11,
        out_specs=[vmem] * len(out_types),
        scratch_shapes=[
            pltpu.SMEM((n_roll,), jnp.int32),
            pltpu.SMEM((n_roll,), jnp.int32),
            vm((2 * tokens, HEAD_WIDTH), full),
            vm((2 * tokens, HEAD_WIDTH), full),
            vm((n_roll, tokens, kv_width), low),
            vm((kv_heads, n_roll, 2, tokens, HEAD_WIDTH), low),
            vm((n_own, n_roll, 2, length, HEAD_WIDTH), low),
            vm((n_own, n_roll, 2, tokens, span), low),
            vm((n_own, n_roll, 2, tokens, span), low),
            vm((n_roll, tokens, q_width), low),
            vm((n_own, n_roll, tokens, span), low),
            vm((rank, q_width), low),
            vm((rank, q_width), low),
            vm((2, rank, n_roll * tokens), low),
            vm((n_roll, rank, 2 * tokens), low),
            vm((2, length, group * 2 * tokens), full),
            vm((length, group * 2 * tokens), low),
            vm((n_own, n_roll, 2, length, HEAD_WIDTH), low),
            vm((n_chips, kv_heads, n_roll, 2, tokens, HEAD_WIDTH), low),
            vm((n_own, n_roll, 2, tokens, span), low),
            vm((n_roll, rank, 2 * tokens), full),
            vm((n_roll, rank, 2 * tokens), full),
            vm((rank, span), full),
            vm((n_own, rank, span), low),
            vm((n_chips, rank, span), low),
            vm((n_own, rank, span), low),
            vm((n_chips, rank, span), low),
            vm((2, rank, span), low),
            vm((2, n_dp, rank, span // n_dp), low),
            vm((2, n_dp, rank, span // n_dp), low),
            dma((8,)),
            dma((kv_heads,)),
            dma((n_own, n_roll)),
            dma((n_own, n_roll)),
            dma((n_own, n_roll, 2, n_chips)),
            dma((n_own, n_roll, n_seq)),
            dma((n_own, n_roll)),
            dma((n_own, n_roll)),
            dma((n_own, n_roll)),
            dma((n_own, n_roll)),
            dma((n_own,)),
            dma((n_own,)),
            dma((2,)),
            dma((2,)),
            dma((n_own, n_roll, n_chips, 2)),
            dma((n_chips, kv_heads, n_roll)),
            dma((n_own, n_roll)),
            dma((n_own, n_roll)),
            dma((2, n_chips)),
            dma((2, n_chips)),
            dma((2, n_dp)),
            dma((2, n_dp)),
            dma((2, n_dp)),
            dma((2, n_dp)),
        ],
        compiler_params=pltpu.CompilerParams(
            collective_id=0, has_side_effects=True, vmem_limit_bytes=VMEM_LIMIT
        ),
    )(
        offsets,
        lengths,
        jnp.asarray(cos_wide),
        jnp.asarray(sin_wide),
        queries,
        unrotated_key_rows,
        value_projection_rows,
        attention_output_gradient,
        normed_hidden_input,
        adapter_down_weight.T,
        adapter_up_weight,
    )
    outs = pl.pallas_call(
        partial(write_kernel, len(out_types)),
        out_shape=[jax.ShapeDtypeStruct(shape, kind) for shape, kind in out_types],
        in_specs=[vmem] * len(out_types),
        out_specs=[anywhere] * len(out_types),
        scratch_shapes=[dma((len(out_types),))],
        compiler_params=pltpu.CompilerParams(vmem_limit_bytes=8 * 1024 * 1024),
    )(*outs)
    grad_query, grad_key, grad_value, grad_down, grad_up = outs
    return (grad_query, grad_key, grad_value, grad_down.T, grad_up)


def dispatch(mesh, *args):
    n_seq = mesh.shape["seq"]
    n_dp = mesh.shape["dp"]
    n_roll, tokens, q_width = args[0].shape
    kv_width = args[1].shape[2]
    kv_heads = kv_width // HEAD_WIDTH
    group = q_width // kv_width
    rows = 2 * tokens * group
    length = n_seq * tokens
    held = 3 * 2 * n_roll * length * kv_width + 10 * n_roll * tokens * q_width
    held = held + 12 * length * rows
    fits = held < VMEM_LIMIT // 2
    whole = kv_heads == n_seq and n_seq % 2 == 0 and 2 * tokens == HEAD_WIDTH
    whole = whole and 2 * tokens >= OFFSET_BOUND and (group * HEAD_WIDTH) % (n_dp * 128) == 0
    if not (fits and whole):
        return on_device(*args)
    return fused_on_device(n_seq, n_dp, *args)


def solution(mesh):
    in_specs = (
        P("dp", "seq", None),
        P("dp", "seq", None),
        P("dp", "seq", None),
        P("dp", "seq", None),
        P("dp", "seq", None),
        P(),
        P(),
        P("dp"),
        P("dp"),
    )
    out_specs = (
        P("dp", "seq", None),
        P("dp", "seq", None),
        P("dp", "seq", None),
        P("seq", None),
        P(None, "seq"),
    )
    return jax.shard_map(
        partial(dispatch, mesh), mesh=mesh, in_specs=in_specs, out_specs=out_specs, check_vma=False
    )
```

```python
from functools import partial

import math

import jax
import jax.numpy as jnp
import numpy as np
from jax import lax
from jax.experimental import pallas as pl
from jax.experimental.pallas import tpu as pltpu
from jax.sharding import PartitionSpec as P

HEAD_WIDTH = 128


rotary_base = 500000.0


def partner_2(value, axis, distance):
    mask = 2**distance
    pairs = [(source, source ^ mask) for source in range(lax.axis_size(axis))]
    return lax.ppermute(value, axis, pairs)


def rotary_tables(length, head_size):
    half_size = head_size // 2
    frequency = rotary_base ** (-(jnp.arange(half_size, dtype=jnp.float32) * 2.0 / head_size))
    angles = jnp.arange(length, dtype=jnp.float32)[:, None] * frequency[None, :]
    return (jnp.cos(angles), jnp.sin(angles))


def rotate(fields, cosine, sine_table, direction):
    half_size = fields.shape[-1] // 2
    first_half = fields[..., :half_size]
    second_half = fields[..., half_size:]
    cos_wide = cosine[:, None, :]
    sin_wide = direction * sine_table[:, None, :]
    return jnp.concatenate(
        [
            first_half * cos_wide - second_half * sin_wide,
            second_half * cos_wide + first_half * sin_wide,
        ],
        axis=-1,
    )


def contract_axes(first_operand, second_operand, first_axis, second_axis):
    return lax.dot_general(
        first_operand,
        second_operand,
        (((first_axis,), (second_axis,)), ((), ())),
        preferred_element_type=jnp.float32,
    )


def block_terms(rot_query, rot_key, value_head, grad_head, offset, begin_row, end_row, score_scale):
    row_index = jnp.arange(begin_row, end_row, dtype=jnp.int32)[:, None]
    col_index = jnp.arange(end_row, dtype=jnp.int32)[None, :]
    visible = (col_index == row_index) | (col_index >= offset) & (col_index <= row_index)
    query_block = rot_query[begin_row:end_row]
    grad_block = grad_head[begin_row:end_row]
    key_block = rot_key[:end_row]
    value_block = value_head[:end_row]
    scores = contract_axes(query_block, key_block, 1, 1) * score_scale
    row_max = jnp.max(jnp.where(visible, scores, -jnp.inf), axis=1, keepdims=True)
    row_total = jnp.sum(jnp.where(visible, jnp.exp(scores - row_max), 0.0), axis=1, keepdims=True)
    grad_prob = contract_axes(grad_block, value_block, 1, 1)
    probability = jnp.where(visible, jnp.exp(scores - row_max), 0.0) / row_total
    row_delta = jnp.sum(probability * grad_prob, axis=1, keepdims=True)
    prob_low = probability.astype(jnp.bfloat16)
    grad_score = (probability * (grad_prob - row_delta) * score_scale).astype(jnp.bfloat16)
    block_grad = jnp.dot(grad_score, key_block, preferred_element_type=jnp.float32)
    key_add = contract_axes(grad_score, query_block, 0, 0)
    value_add = contract_axes(prob_low, grad_block, 0, 0)
    return (block_grad, key_add, value_add)


def head_backward(rot_query, rot_key, value_head, grad_head, offset, block_rows):
    length = rot_query.shape[0]
    head_size = rot_query.shape[1]
    score_scale = head_size ** (-0.5)
    query_parts = []
    key_terms = []
    value_terms = []
    for block_index in range(length // block_rows):
        begin_row = block_index * block_rows
        end_row = begin_row + block_rows
        live_terms = partial(
            block_terms,
            rot_query,
            rot_key,
            value_head,
            grad_head,
            offset,
            begin_row,
            end_row,
            score_scale,
        )
        results = live_terms()
        block_grad, key_add, value_add = results
        query_parts.append(block_grad)
        key_terms.append(jnp.pad(key_add, ((0, length - end_row), (0, 0))))
        value_terms.append(jnp.pad(value_add, ((0, length - end_row), (0, 0))))
    key_accum = key_terms[0]
    value_accum = value_terms[0]
    for term_index in range(1, len(key_terms)):
        key_accum = key_accum + key_terms[term_index]
        value_accum = value_accum + value_terms[term_index]
    return (jnp.concatenate(query_parts, axis=0), key_accum, value_accum)


def arrange_rows(rows, share, part_rows, key_groups):
    rollout_count = rows.shape[0]
    split = rows.reshape(rollout_count, share, part_rows, key_groups, HEAD_WIDTH)
    return jnp.transpose(split, (0, 2, 3, 1, 4)).reshape(
        rollout_count, part_rows, key_groups * share, HEAD_WIDTH
    )


def join_group(paired, share, seq_parts, part_rows):
    my_index = lax.axis_index("seq")
    rollout_count = paired.shape[1]
    local_keys = paired.shape[3]
    joined = paired[None]
    for bit in range(share.bit_length() - 1):
        partner = partner_2(joined, "seq", bit)
        upper = my_index // (1 << bit) % 2
        joined = jnp.where(
            upper == 0,
            jnp.concatenate([joined, partner], axis=0),
            jnp.concatenate([partner, joined], axis=0),
        )
    ordered = joined.reshape(share, 2, rollout_count, seq_parts, part_rows, local_keys, HEAD_WIDTH)
    ordered = jnp.transpose(ordered, (1, 2, 3, 0, 4, 5, 6))
    return ordered.reshape(2, rollout_count, seq_parts * share * part_rows, local_keys, HEAD_WIDTH)


def reduce_group(partial_sums, share, seq_parts, part_rows):
    my_index = lax.axis_index("seq")
    rollout_count = partial_sums.shape[1]
    local_keys = partial_sums.shape[3]
    split = partial_sums.reshape(
        2, rollout_count, seq_parts, share, part_rows, local_keys, HEAD_WIDTH
    )
    split = jnp.transpose(split, (3, 0, 1, 2, 4, 5, 6))
    for bit in reversed(range(share.bit_length() - 1)):
        half = split.shape[0] // 2
        lower_half = split[:half]
        upper_half = split[half:]
        upper = my_index // (1 << bit) % 2
        keep = jnp.where(upper == 0, lower_half, upper_half)
        outgoing = jnp.where(upper == 0, upper_half, lower_half)
        split = keep + partner_2(outgoing.astype(jnp.bfloat16), "seq", bit).astype(outgoing.dtype)
    return split[0].reshape(2, rollout_count, seq_parts * part_rows, local_keys, HEAD_WIDTH)


def on_device(
    queries,
    unrotated_key_rows,
    value_projection_rows,
    attention_output_gradient,
    normed_hidden_input,
    adapter_down_weight,
    adapter_up_weight,
    lengths,
    offsets,
):
    rollout_count = queries.shape[0]
    tokens = queries.shape[1]
    seq_parts = lax.axis_size("seq")
    length = tokens * seq_parts
    query_width = queries.shape[2]
    head_count = query_width // HEAD_WIDTH
    key_groups = unrotated_key_rows.shape[2] // HEAD_WIDTH
    local_heads = head_count // seq_parts
    adapter_rank_size = adapter_down_weight.shape[1]
    share = max(1, seq_parts // key_groups)
    part_rows = tokens // share
    query_tokens = queries.reshape(rollout_count, tokens, head_count, HEAD_WIDTH)
    grad_tokens = attention_output_gradient.reshape(rollout_count, tokens, head_count, HEAD_WIDTH)
    key_arranged = arrange_rows(unrotated_key_rows, share, part_rows, key_groups)
    value_arranged = arrange_rows(value_projection_rows, share, part_rows, key_groups)
    query_heads, key_parted, value_parted, grad_heads = (
        lax.all_to_all(query_tokens, "seq", split_axis=2, concat_axis=1, tiled=True),
        lax.all_to_all(key_arranged, "seq", split_axis=2, concat_axis=1, tiled=True),
        lax.all_to_all(value_arranged, "seq", split_axis=2, concat_axis=1, tiled=True),
        lax.all_to_all(grad_tokens, "seq", split_axis=2, concat_axis=1, tiled=True),
    )
    paired = join_group(jnp.stack([key_parted, value_parted], axis=0), share, seq_parts, part_rows)
    key_heads = paired[0]
    value_heads = paired[1]
    local_keys = key_heads.shape[2]
    cosine, sine_table = rotary_tables(length, HEAD_WIDTH)
    positions = jnp.arange(length, dtype=jnp.int32)
    keep_mask = (positions[None, :] >= offsets[:, None]) & (positions[None, :] < lengths[:, None])
    grad_heads = jnp.where(keep_mask[:, :, None, None], grad_heads, jnp.zeros_like(grad_heads))
    rot_query = rotate(query_heads.astype(jnp.float32), cosine, sine_table, 1.0).astype(
        jnp.bfloat16
    )
    rot_key = rotate(key_heads.astype(jnp.float32), cosine, sine_table, 1.0).astype(jnp.bfloat16)
    block_rows = min(512, length)
    query_rolls = []
    key_rolls = []
    value_rolls = []
    for rollout_slot in range(rollout_count):
        query_list = []
        key_list = []
        value_list = []
        for head_slot in range(local_heads):
            key_slot = head_slot * local_keys // local_heads
            query_grad, key_grad, value_grad = head_backward(
                rot_query[rollout_slot, :, head_slot],
                rot_key[rollout_slot, :, key_slot],
                value_heads[rollout_slot, :, key_slot],
                grad_heads[rollout_slot, :, head_slot],
                offsets[rollout_slot],
                block_rows,
            )
            query_list.append(
                rotate(query_grad[:, None, :], cosine, sine_table, -1.0)[:, 0].astype(jnp.bfloat16)
            )
            key_list.append(
                rotate(key_grad[:, None, :], cosine, sine_table, -1.0)[:, 0].astype(jnp.bfloat16)
            )
            value_list.append(value_grad.astype(jnp.bfloat16))
        query_rolls.append(jnp.stack(query_list, axis=1))
        key_rolls.append(jnp.stack(key_list, axis=1))
        value_rolls.append(jnp.stack(value_list, axis=1))
    query_back = jnp.stack(query_rolls, axis=0)
    key_parts = jnp.stack(key_rolls, axis=0)
    value_parts = jnp.stack(value_rolls, axis=0)
    shared_heads = local_heads // local_keys
    key_local = (
        key_parts.astype(jnp.float32)
        .reshape(rollout_count, length, local_keys, shared_heads, HEAD_WIDTH)
        .sum(axis=3)
    )
    value_local = (
        value_parts.astype(jnp.float32)
        .reshape(rollout_count, length, local_keys, shared_heads, HEAD_WIDTH)
        .sum(axis=3)
    )
    summed = reduce_group(
        jnp.stack([key_local, value_local], axis=0), share, seq_parts, part_rows
    ).astype(jnp.bfloat16)
    query_result, key_result, value_result = (
        lax.all_to_all(query_back, "seq", split_axis=1, concat_axis=2, tiled=True),
        lax.all_to_all(summed[0], "seq", split_axis=1, concat_axis=2, tiled=True),
        lax.all_to_all(summed[1], "seq", split_axis=1, concat_axis=2, tiled=True),
    )
    key_total = jnp.transpose(
        key_result.reshape(rollout_count, part_rows, key_groups, share, HEAD_WIDTH), (0, 3, 1, 2, 4)
    ).reshape(rollout_count, tokens, key_groups * HEAD_WIDTH)
    value_total = jnp.transpose(
        value_result.reshape(rollout_count, part_rows, key_groups, share, HEAD_WIDTH),
        (0, 3, 1, 2, 4),
    ).reshape(rollout_count, tokens, key_groups * HEAD_WIDTH)
    flattened_query = query_result.reshape(rollout_count * tokens, query_width)
    hidden_state = normed_hidden_input.reshape(rollout_count * tokens, normed_hidden_input.shape[2])
    adapter_latent = jnp.dot(
        hidden_state, adapter_down_weight, preferred_element_type=jnp.float32
    ).astype(jnp.bfloat16)
    backward_gradient = contract_axes(flattened_query, adapter_up_weight, 1, 1).astype(jnp.bfloat16)
    joined_terms = lax.psum_scatter(
        jnp.concatenate(
            [
                contract_axes(hidden_state, backward_gradient, 0, 0),
                contract_axes(flattened_query, adapter_latent, 0, 0),
            ],
            axis=1,
        ).astype(jnp.bfloat16),
        "seq",
        scatter_dimension=0,
        tiled=True,
    ).astype(jnp.float32)
    down_local = joined_terms[:, :adapter_rank_size]
    up_local = joined_terms[:, adapter_rank_size:]
    down_sum, up_sum = (
        lax.psum(down_local.astype(jnp.bfloat16), "dp").astype(jnp.float32),
        lax.psum(up_local.astype(jnp.bfloat16), "dp").astype(jnp.float32),
    )
    return (
        flattened_query.reshape(rollout_count, tokens, query_width),
        key_total,
        value_total,
        down_sum,
        up_sum.T,
    )


VMEM_LIMIT = 48 * 1024 * 1024
MERGE_LAG = 3
HELD = 3
SEND_AHEAD = 2
NEG = -1e30
OFFSET_BOUND = 32


def nt_dot(left, right):
    return lax.dot_general(
        left, right, (((1,), (1,)), ((), ())), preferred_element_type=jnp.float32
    )


def fused_kernel(
    n_seq,
    n_dp,
    n_roll,
    tokens,
    kv_heads,
    group,
    rank,
    off_hbm,
    len_hbm,
    cos_hbm,
    sin_hbm,
    q_hbm,
    k_hbm,
    v_hbm,
    g_hbm,
    hid_hbm,
    down_hbm,
    up_hbm,
    gq_ref,
    gk_ref,
    gv_ref,
    gd_ref,
    gu_ref,
    off_ref,
    len_ref,
    cos_ref,
    sin_ref,
    k_raw,
    kv_own,
    kv_all,
    q_all,
    g_all,
    hid_own,
    hid_other,
    down_ref,
    up_ref,
    lat_all,
    lat_roll,
    score_buf,
    prob_buf,
    dkv_own,
    dkv_all,
    gq_all,
    back_acc,
    back_got,
    up_acc,
    up_own,
    up_got,
    dn_own,
    dn_got,
    z_own,
    z_got,
    z_all,
    merge_buf,
    relay_buf,
    loc_sem,
    v_sem,
    ql_sem,
    gl_sem,
    kv_send,
    kv_recv,
    q_send,
    q_recv,
    g_send,
    g_recv,
    hid_send,
    hid_recv,
    one_send,
    one_recv,
    dk_send,
    dk_recv,
    gq_send,
    gq_recv,
    ad_send,
    ad_recv,
    rs_send,
    rs_recv,
    ag_send,
    ag_recv,
    fw_send,
    mg_send,
    mg_recv,
    rl_send,
    rl_recv,
):
    me = lax.axis_index("seq")
    my_dp = lax.axis_index("dp")
    chip = me // 2
    core = me % 2
    partner = me + 1 - 2 * core
    n_chips = n_seq // 2
    n_own = kv_heads // 2
    width = HEAD_WIDTH
    half = width // 2
    span = group * width
    chip_tokens = 2 * tokens
    rows = group * chip_tokens
    scale = width ** (-0.5)
    exp_scale = scale * math.log2(math.e)
    piece = span // n_dp
    n_units = n_own * n_roll

    def lanes(index, size):
        return pl.ds(pl.multiple_of(index * size, size), size)

    def seq_rows(device):
        return pl.ds(pl.multiple_of(device * tokens, tokens), tokens)

    def local(src, dst, sem):
        return pltpu.make_async_copy(src, dst, sem)

    def remote(src, dst, send, recv, where):
        return pltpu.make_async_remote_copy(
            src_ref=src, dst_ref=dst, send_sem=send, recv_sem=recv, device_id=where
        )

    def each_unit(body):
        def step(index, carry):
            body(index // n_roll, index % n_roll)
            return carry

        lax.fori_loop(0, n_own * n_roll, step, 0)

    barrier = pltpu.get_barrier_semaphore()
    for step in range(1, n_seq):
        pl.semaphore_signal(barrier, inc=1, device_id={"seq": lax.rem(me + step, n_seq)})
    for step in range(1, n_dp):
        pl.semaphore_signal(barrier, inc=1, device_id={"dp": lax.rem(my_dp + step, n_dp)})

    chip_rows = pl.ds(pl.multiple_of(chip * chip_tokens, chip_tokens), chip_tokens)
    k_load = local(k_hbm, k_raw, loc_sem.at[0])
    cos_load = local(cos_hbm.at[chip_rows], cos_ref, loc_sem.at[1])
    sin_load = local(sin_hbm.at[chip_rows], sin_ref, loc_sem.at[2])
    off_load = local(off_hbm, off_ref, loc_sem.at[3])
    len_load = local(len_hbm, len_ref, loc_sem.at[4])
    hid_load = local(hid_hbm, hid_own, loc_sem.at[5])
    down_load = local(down_hbm, down_ref, loc_sem.at[6])
    up_load = local(up_hbm, up_ref, loc_sem.at[7])

    def v_load(h):
        return local(v_hbm.at[:, :, lanes(h, width)], kv_own.at[h, :, 1], v_sem.at[h])

    def q_load(i, r):
        h = 2 * i + core
        return local(q_hbm.at[r, :, lanes(h, span)], q_all.at[i, r, core], ql_sem.at[i, r])

    def g_load(i, r):
        h = 2 * i + core
        return local(g_hbm.at[r, :, lanes(h, span)], g_all.at[i, r, core], gl_sem.at[i, r])

    def load_queries(i, r):
        q_load(i, r).start()
        g_load(i, r).start()

    k_load.start()
    cos_load.start()
    sin_load.start()
    for h in range(kv_heads):
        v_load(h).start()
    off_load.start()
    len_load.start()
    each_unit(load_queries)
    hid_load.start()
    down_load.start()
    up_load.start()

    def q_copy(i, r):
        h = 2 * i + 1 - core
        return remote(
            q_hbm.at[r, :, lanes(h, span)],
            q_all.at[i, r, core],
            q_send.at[i, r],
            q_recv.at[i, r],
            {"seq": partner},
        )

    def g_copy(i, r):
        h = 2 * i + 1 - core
        return remote(
            g_hbm.at[r, :, lanes(h, span)],
            g_all.at[i, r, core],
            g_send.at[i, r],
            g_recv.at[i, r],
            {"seq": partner},
        )

    def hid_copy(i):
        h = 2 * i + 1 - core
        return remote(
            hid_hbm.at[:, :, lanes(h, span)],
            hid_other.at[i],
            hid_send.at[i],
            hid_recv.at[i],
            {"seq": partner},
        )

    def send_queries(i, r):
        q_copy(i, r).start()
        g_copy(i, r).start()

    def gather_copy(i, r, parity, chip_step):
        h = 2 * i + parity
        return remote(
            kv_own.at[h, r],
            kv_all.at[i, r, :, seq_rows(me), :],
            kv_send.at[i, r, parity, chip_step],
            kv_recv.at[i, r, me],
            {"seq": 2 * (chip + chip_step) + parity},
        )

    def pair_copy(i, r):
        h = 2 * i + 1 - core
        return remote(
            kv_own.at[h, r],
            kv_all.at[i, r, :, seq_rows(me), :],
            kv_send.at[i, r, 0, 0],
            kv_recv.at[i, r, me],
            {"seq": partner},
        )

    n_passed = n_own // 2

    def gather_ops(i, r, act, later=False):
        if not later:
            act(pair_copy(i, r))
        for chip_step in range(1, n_chips):
            mine = chip + chip_step < n_chips
            if chip_step == 3:
                mine = mine & (i >= n_passed)
            if chip_step == 1:
                mine = mine & ((chip == 1) if later else (chip != 1))
            elif later:
                continue

            @pl.when(mine)
            def _():
                for parity in range(2):
                    act(gather_copy(i, r, parity, chip_step))

    def later_ops(index, act):
        @pl.when((chip == 1) & (index >= n_passed * n_roll) & (index < n_units))
        def _():
            gather_ops(index // n_roll, index % n_roll, act, later=True)

    def gather_got(i, r, device):
        return remote(
            kv_own.at[0, r],
            kv_all.at[i, r, :, seq_rows(device), :],
            kv_send.at[i, r, 0, 0],
            kv_recv.at[i, r, device],
            {"seq": partner},
        )

    def pass_copy(i, r, source_core):
        source = 2 * (chip - 2) + source_core
        return remote(
            kv_all.at[i, r, :, seq_rows(source), :],
            kv_all.at[i, r, :, seq_rows(source), :],
            fw_send.at[i, r, source_core],
            kv_recv.at[i, r, source],
            {"seq": 2 * (5 - chip) + core},
        )

    def pass_on(index, carry):
        i = index // n_roll
        r = index % n_roll
        gather_ops(i, r, lambda copy: copy.start())

        @pl.when(i < n_passed)
        def _():
            for source_core in range(2):
                gather_got(i, r, 2 * (chip - 2) + source_core).wait_recv()
                pass_copy(i, r, source_core).start()

        return carry

    def passed_sent(i, r):
        @pl.when((chip >= 2) & (i < n_passed))
        def _():
            for source_core in range(2):
                pass_copy(i, r, source_core).wait_send()

    def gather_wait(i, r):
        def block(source):
            for source_core in range(2):
                gather_got(i, r, 2 * source + source_core).wait_recv()

        gather_got(i, r, partner).wait_recv()

        @pl.when((chip == 1) | ((chip >= 2) & (i >= n_passed)))
        def _():
            block(0)

        @pl.when((chip >= 2) & (i >= n_passed))
        def _():
            block(1)

        @pl.when((chip == 2) & (i < n_passed))
        def _():
            block(1)

        @pl.when((chip == 3) & (i < n_passed))
        def _():
            block(0)

        @pl.when(chip == 3)
        def _():
            block(2)

    def reduce_copy(i, r, target_chip, target_core):
        target = 2 * target_chip + target_core
        return remote(
            dkv_own.at[i, r, :, seq_rows(target), :],
            dkv_all.at[chip, 2 * i + core, r],
            dk_send.at[i, r, target_chip, target_core],
            dk_recv.at[chip, 2 * i + core, r],
            {"seq": target},
        )

    def chip_block(target_chip):
        return pl.ds(target_chip * chip_tokens, chip_tokens)

    def merge_copy(i, r, target_chip):
        return remote(
            dkv_own.at[i, r, :, chip_block(0), :],
            merge_buf.at[i, r],
            mg_send.at[i, r],
            mg_recv.at[i, r],
            {"seq": 2 * target_chip + core},
        )

    def relay_copy(i, r):
        return remote(
            dkv_own.at[i, r, :, chip_block(1), :],
            relay_buf.at[i, r],
            rl_send.at[i, r],
            rl_recv.at[i, r],
            {"seq": core},
        )

    def pass_back_copy(i, r, target_core):
        return remote(
            relay_buf.at[i, r, :, pl.ds(target_core * tokens, tokens), :],
            dkv_all.at[2, 2 * i + core, r],
            dk_send.at[i, r, 1, target_core],
            dk_recv.at[2, 2 * i + core, r],
            {"seq": 2 + target_core},
        )

    def merges(r):
        return ((chip == 1) & (r % 2 == 0)) | ((chip == 2) & (r % 2 == 1))

    def block_ops(i, r, target_chip, act):
        for target_core in range(2):
            act(reduce_copy(i, r, target_chip, target_core))

    def reduce_ops(i, r, act):
        act(reduce_copy(i, r, chip, 1 - core))
        index = i * n_roll + r

        @pl.when(((chip == 1) | (chip == 2)) & ~merges(r))
        def _():
            block_ops(i, r, 0, act)

        @pl.when((chip == 2) & (i < n_passed))
        def _():
            act(relay_copy(i, r))

        @pl.when((chip == 3) & (index < n_units - HELD))
        def _():
            top_ops(i, r, act)

    def top_ops(i, r, act):
        for route in range(2):

            @pl.when(r % 2 == route)
            def _():
                act(merge_copy(i, r, 1 + route))

        block_ops(i, r, 2, act)
        block_ops(i, r, 1, act)

    def held_ops(i, r, act):
        @pl.when((chip == 2) & (i >= n_passed))
        def _():
            block_ops(i, r, 1, act)

        @pl.when((chip == 3) & (i * n_roll + r >= n_units - HELD))
        def _():
            top_ops(i, r, act)

    def merge(i, r):
        @pl.when(merges(r))
        def _():
            merge_copy(i, r, 0).wait_recv()
            for t in range(2):
                block = dkv_own[i, r, t, :chip_tokens, :].astype(jnp.float32)
                block = block + merge_buf[i, r, t].astype(jnp.float32)
                dkv_own[i, r, t, :chip_tokens, :] = block.astype(jnp.bfloat16)
            block_ops(i, r, 0, lambda copy: copy.start())

    def pass_back(i, r):
        relay_copy(i, r).wait_recv()
        for target_core in range(2):
            pass_back_copy(i, r, target_core).start()

    def reduce_got(source, h, r):
        return remote(
            dkv_own.at[0, 0, :, pl.ds(0, tokens), :],
            dkv_all.at[source, h, r],
            dk_send.at[0, 0, 0, 0],
            dk_recv.at[source, h, r],
            {"seq": partner},
        )

    def gq_copy(i, r, parity):
        return remote(
            gq_all.at[i, r, 1 - core],
            gq_ref.at[r, :, lanes(2 * i + parity, span)],
            gq_send.at[i, r],
            gq_recv.at[i, r],
            {"seq": partner},
        )

    def adapter_copy(t, own, got, source, target_chip):
        return remote(
            own.at[target_chip],
            got.at[source],
            ad_send.at[t, target_chip],
            ad_recv.at[t, source],
            {"seq": 2 * target_chip + core},
        )

    k_load.wait()
    cos_load.wait()
    sin_load.wait()
    own_rows = pl.ds(pl.multiple_of(core * tokens, tokens), tokens)
    cos_own = cos_ref[own_rows, :]
    sin_own = sin_ref[own_rows, :]
    for h in range(kv_heads):
        for r in range(n_roll):
            key = k_raw[r, :, h * width : (h + 1) * width].astype(jnp.float32)
            key = key * cos_own + pltpu.roll(key, half, 1) * sin_own
            kv_own[h, r, 0] = key.astype(jnp.bfloat16)
    for h in range(kv_heads):
        v_load(h).wait()
    for i in range(n_own):
        for r in range(n_roll):
            kv_all[i, r, :, seq_rows(me), :] = kv_own[2 * i + core, r]

    pl.semaphore_wait(barrier, n_seq + n_dp - 2)

    @pl.when(chip < 2)
    def _():
        each_unit(lambda i, r: gather_ops(i, r, lambda copy: copy.start()))

    each_unit(send_queries)

    hid_load.wait()
    down_load.wait()
    flat = n_roll * tokens
    hid_rows = hid_own[...].reshape(flat, hid_own.shape[2])
    lat_all[core] = nt_dot(down_ref[...], hid_rows).astype(jnp.bfloat16)
    lat_copy = remote(
        lat_all.at[core], lat_all.at[core], one_send.at[0], one_recv.at[0], {"seq": partner}
    )
    lat_copy.start()
    for i in range(n_own):
        hid_copy(i).start()

    @pl.when(chip >= 2)
    def _():
        lax.fori_loop(0, n_units, pass_on, 0)

    back_acc[...] = jnp.zeros_like(back_acc)
    up_acc[...] = jnp.zeros_like(up_acc)
    up_load.wait()
    off_load.wait()
    len_load.wait()
    remote(
        lat_all.at[core], lat_all.at[1 - core], one_send.at[0], one_recv.at[0], {"seq": partner}
    ).wait_recv()
    for r in range(n_roll):
        lane = slice(r * tokens, (r + 1) * tokens)
        lat_roll[r] = jnp.concatenate([lat_all[0, :, lane], lat_all[1, :, lane]], axis=1)

    def attend(i, r, blocks):
        n_keys = blocks * chip_tokens
        offset = off_ref[r]
        position = chip * chip_tokens + lax.broadcasted_iota(jnp.int32, (chip_tokens, width), 0)
        keep = (position >= offset) & (position < len_ref[r])
        cos = cos_ref[...]
        sin = sin_ref[...]
        queries = []
        grads = []
        for j in range(group):
            lane = slice(j * width, (j + 1) * width)
            query = q_all[i, r, :, :, lane].reshape(chip_tokens, width).astype(jnp.float32)
            query = query * cos + pltpu.roll(query, half, 1) * sin
            queries.append(query.astype(jnp.bfloat16))
            grad = g_all[i, r, :, :, lane].reshape(chip_tokens, width).astype(jnp.float32)
            grads.append(jnp.where(keep, grad, 0.0).astype(jnp.bfloat16))
        query = jnp.concatenate(queries, axis=0)
        grad = jnp.concatenate(grads, axis=0)
        key = kv_all[i, r, 0, :n_keys, :]

        row_max = None
        for b in range(blocks):
            keys = slice(b * chip_tokens, (b + 1) * chip_tokens)
            score = nt_dot(kv_all[i, r, 0, keys, :], query)
            if b == blocks - 1 or b * chip_tokens < OFFSET_BOUND:
                key_row = lax.broadcasted_iota(jnp.int32, (chip_tokens, rows), 0)
                visible = key_row + b * chip_tokens >= offset
                if b == blocks - 1:
                    query_row = lax.broadcasted_iota(jnp.int32, (chip_tokens, rows), 1) % chip_tokens
                    visible = (key_row == query_row) | (visible & (key_row <= query_row))
                score = jnp.where(visible, score, NEG)
            score_buf[0, keys, :] = score
            part = jnp.max(score, axis=0, keepdims=True)
            row_max = part if row_max is None else jnp.maximum(row_max, part)
        total = None
        delta = None
        for b in range(blocks):
            keys = slice(b * chip_tokens, (b + 1) * chip_tokens)
            weight = jnp.exp2((score_buf[0, keys, :] - row_max) * exp_scale)
            grad_prob = nt_dot(kv_all[i, r, 1, keys, :], grad)
            score_buf[0, keys, :] = weight
            score_buf[1, keys, :] = grad_prob
            part = jnp.sum(weight, axis=0, keepdims=True)
            total = part if total is None else total + part
            part = jnp.sum(weight * grad_prob, axis=0, keepdims=True)
            delta = part if delta is None else delta + part
        inverse = 1.0 / total
        delta = delta * inverse
        inverse_scaled = inverse * scale
        for b in range(blocks):
            keys = slice(b * chip_tokens, (b + 1) * chip_tokens)
            weight = score_buf[0, keys, :]
            prob = (weight * inverse).astype(jnp.bfloat16)
            slope = ((weight * inverse_scaled) * (score_buf[1, keys, :] - delta)).astype(jnp.bfloat16)
            prob_buf[keys, :] = slope
            dkv_own[i, r, 1, keys, :] = jnp.dot(
                prob, grad, preferred_element_type=jnp.float32
            ).astype(jnp.bfloat16)
            dkv_own[i, r, 0, keys, :] = jnp.dot(
                slope, query, preferred_element_type=jnp.float32
            ).astype(jnp.bfloat16)
        back = jnp.dot(key.T, prob_buf[:n_keys, :], preferred_element_type=jnp.float32).T
        for j in range(group):
            part = back[j * chip_tokens : (j + 1) * chip_tokens]
            part = part * cos - pltpu.roll(part, half, 1) * sin
            part = part.astype(jnp.bfloat16).reshape(2, tokens, width)
            gq_all[i, r, :, :, j * width : (j + 1) * width] = part

    def unit(i, r):
        h = 2 * i + core
        gather_wait(i, r)
        later_ops(i * n_roll + r + SEND_AHEAD, lambda copy: copy.start())
        q_load(i, r).wait()
        g_load(i, r).wait()
        remote(
            q_hbm.at[r, :, lanes(h, span)],
            q_all.at[i, r, 1 - core],
            q_send.at[i, r],
            q_recv.at[i, r],
            {"seq": partner},
        ).wait_recv()
        remote(
            g_hbm.at[r, :, lanes(h, span)],
            g_all.at[i, r, 1 - core],
            g_send.at[i, r],
            g_recv.at[i, r],
            {"seq": partner},
        ).wait_recv()
        for blocks in range(1, n_chips + 1):

            @pl.when(chip == blocks - 1)
            def _():
                attend(i, r, blocks)

        reduce_ops(i, r, lambda copy: copy.start())
        gq_copy(i, r, core).start()
        late = i * n_roll + r - MERGE_LAG

        @pl.when(late >= 0)
        def _():
            merge(late // n_roll, late % n_roll)

        dkv_all[chip, h, r] = dkv_own[i, r, :, seq_rows(me), :]
        gq_ref[r, :, lanes(h, span)] = gq_all[i, r, core]
        grad_query = gq_all[i, r].reshape(chip_tokens, span)
        back_acc[r] = back_acc[r] + nt_dot(up_ref[:, lanes(h, span)], grad_query)
        up_part = jnp.dot(lat_roll[r], grad_query, preferred_element_type=jnp.float32)
        up_total = jnp.where(r == 0, 0.0, up_acc[...]) + up_part
        up_acc[...] = up_total

        @pl.when(r == n_roll - 1)
        def _():
            up_own[i] = up_total.astype(jnp.bfloat16)

            @pl.when(i != chip)
            def _():
                adapter_copy(1, up_own, up_got, chip, i).start()

    each_unit(unit)

    back_copy = remote(back_acc, back_got, one_send.at[1], one_recv.at[1], {"seq": partner})
    back_copy.start()
    for i in range(n_own):
        hid_copy(i).wait_recv()
    back_copy.wait_recv()
    sums = [(back_acc[r] + back_got[r]).astype(jnp.bfloat16) for r in range(n_roll)]
    first = jnp.concatenate([part[:, :tokens] for part in sums], axis=1)
    second = jnp.concatenate([part[:, tokens:] for part in sums], axis=1)
    back_own = jnp.where(core == 0, first, second)
    back_other = jnp.where(core == 0, second, first)
    for i in range(n_own):
        own = hid_own[:, :, lanes(2 * i + core, span)].reshape(flat, span)
        other = hid_other[i].reshape(flat, span)
        dn_own[i] = (
            jnp.dot(back_own, own, preferred_element_type=jnp.float32)
            + jnp.dot(back_other, other, preferred_element_type=jnp.float32)
        ).astype(jnp.bfloat16)

        @pl.when(i != chip)
        def _():
            adapter_copy(0, dn_own, dn_got, chip, i).start()

    def owner_sum(t, own, got):
        total = own[chip].astype(jnp.float32)
        for step in range(1, n_chips):
            source = lax.rem(chip + step, n_chips)
            adapter_copy(t, own, got, source, 0).wait_recv()
            total = total + got[source].astype(jnp.float32)
        z_own[t] = total.astype(jnp.bfloat16)

    def scatter_copy(t, target):
        return remote(
            z_own.at[t, :, lanes(target, piece)],
            z_got.at[t, my_dp],
            rs_send.at[t, target],
            rs_recv.at[t, my_dp],
            {"dp": target},
        )

    def scatter_start(t):
        for step in range(1, n_dp):
            scatter_copy(t, lax.rem(my_dp + step, n_dp)).start()

    def collect_copy(t, target):
        return remote(
            z_all.at[t, my_dp],
            z_all.at[t, my_dp],
            ag_send.at[t, target],
            ag_recv.at[t, my_dp],
            {"dp": target},
        )

    def collect_start(t):
        total = z_own[t, :, lanes(my_dp, piece)].astype(jnp.float32)
        for step in range(1, n_dp):
            source = lax.rem(my_dp + step, n_dp)
            remote(
                z_own.at[t, :, lanes(source, piece)],
                z_got.at[t, source],
                rs_send.at[t, source],
                rs_recv.at[t, source],
                {"dp": source},
            ).wait_recv()
            total = total + z_got[t, source].astype(jnp.float32)
        z_all[t, my_dp] = total.astype(jnp.bfloat16)
        for step in range(1, n_dp):
            collect_copy(t, lax.rem(my_dp + step, n_dp)).start()

    def collect_out(t, out):
        for step in range(1, n_dp):
            source = lax.rem(my_dp + step, n_dp)
            remote(
                z_all.at[t, source],
                z_all.at[t, source],
                ag_send.at[t, source],
                ag_recv.at[t, source],
                {"dp": source},
            ).wait_recv()
        for d in range(n_dp):
            out[:, d * piece : (d + 1) * piece] = z_all[t, d].astype(jnp.float32)

    each_unit(lambda i, r: held_ops(i, r, lambda copy: copy.start()))

    @pl.when(chip == 0)
    def _():
        for i in range(n_passed):
            for r in range(n_roll):
                pass_back(i, r)

    owner_sum(1, up_own, up_got)
    scatter_start(1)

    cos_own = cos_ref[own_rows, :]
    sin_own = sin_ref[own_rows, :]

    n_sources = jnp.where(chip == 0, n_chips - 1, n_chips)

    def finish(h, r):
        @pl.when(h % 2 != core)
        def _():
            reduce_got(chip, h, r).wait_recv()

        for source in range(1, n_chips):

            @pl.when((source > chip) & (source < n_sources))
            def _():
                reduce_got(source, h, r).wait_recv()

        def add(source, totals):
            return tuple(
                totals[t] + dkv_all[source, h, r, t].astype(jnp.float32) for t in range(2)
            )

        first = tuple(dkv_all[chip, h, r, t].astype(jnp.float32) for t in range(2))
        key, value = lax.fori_loop(chip + 1, n_sources, add, first)
        key = key * cos_own - pltpu.roll(key, half, 1) * sin_own
        gk_ref[r, :, lanes(h, width)] = key.astype(jnp.bfloat16)
        gv_ref[r, :, lanes(h, width)] = value.astype(jnp.bfloat16)

    def finish_step(index, carry):
        finish(index // n_roll, index % n_roll)
        return carry

    early = (kv_heads - 4) * n_roll
    lax.fori_loop(0, early, finish_step, 0)
    collect_start(1)
    owner_sum(0, dn_own, dn_got)
    scatter_start(0)
    collect_out(1, gu_ref)
    each_unit(lambda i, r: gq_copy(i, r, 1 - core).wait_recv())
    collect_start(0)

    def merge_step(index, carry):
        merge(index // n_roll, index % n_roll)
        return carry

    lax.fori_loop(max(0, n_units - MERGE_LAG), n_units, merge_step, 0)

    lax.fori_loop(early, kv_heads * n_roll, finish_step, 0)

    each_unit(lambda i, r: gather_ops(i, r, lambda copy: copy.wait_send()))
    each_unit(lambda i, r: later_ops(i * n_roll + r, lambda copy: copy.wait_send()))
    each_unit(lambda i, r: reduce_ops(i, r, lambda copy: copy.wait_send()))
    each_unit(lambda i, r: held_ops(i, r, lambda copy: copy.wait_send()))
    each_unit(passed_sent)

    def merged_sent(i, r):
        @pl.when(merges(r))
        def _():
            block_ops(i, r, 0, lambda copy: copy.wait_send())

        @pl.when((chip == 0) & (i < n_passed))
        def _():
            for target_core in range(2):
                pass_back_copy(i, r, target_core).wait_send()

    each_unit(merged_sent)

    def sent(i, r):
        q_copy(i, r).wait_send()
        g_copy(i, r).wait_send()
        gq_copy(i, r, core).wait_send()

    each_unit(sent)
    lat_copy.wait_send()
    back_copy.wait_send()
    for i in range(n_own):
        hid_copy(i).wait_send()

        @pl.when(i != chip)
        def _():
            adapter_copy(0, dn_own, dn_got, chip, i).wait_send()
            adapter_copy(1, up_own, up_got, chip, i).wait_send()

    collect_out(0, gd_ref)
    for t in range(2):
        for step in range(1, n_dp):
            target = lax.rem(my_dp + step, n_dp)
            scatter_copy(t, target).wait_send()
            collect_copy(t, target).wait_send()


def write_kernel(n_outs, *refs):
    sem = refs[2 * n_outs]
    copies = [
        pltpu.make_async_copy(refs[n], refs[n_outs + n], sem.at[n]) for n in range(n_outs)
    ]
    for copy in copies:
        copy.start()
    for copy in copies:
        copy.wait()


def fused_on_device(
    n_seq,
    n_dp,
    queries,
    unrotated_key_rows,
    value_projection_rows,
    attention_output_gradient,
    normed_hidden_input,
    adapter_down_weight,
    adapter_up_weight,
    lengths,
    offsets,
):
    n_roll, tokens, q_width = queries.shape
    kv_width = unrotated_key_rows.shape[2]
    kv_heads = kv_width // HEAD_WIDTH
    group = q_width // kv_width
    rank = adapter_down_weight.shape[1]
    length = n_seq * tokens
    n_chips = n_seq // 2
    n_own = kv_heads // 2
    half = HEAD_WIDTH // 2
    frequency = rotary_base ** (-(np.arange(half, dtype=np.float32) * 2.0 / HEAD_WIDTH))
    angles = np.arange(length, dtype=np.float32)[:, None] * frequency.astype(np.float32)[None, :]
    cosine, sine = np.cos(angles), np.sin(angles)
    cos_wide = np.concatenate([cosine, cosine], axis=1).astype(np.float32)
    sin_wide = np.concatenate([-sine, sine], axis=1).astype(np.float32)
    span = q_width // n_seq
    low = jnp.bfloat16
    full = jnp.float32
    dma = pltpu.SemaphoreType.DMA
    vm = pltpu.VMEM
    anywhere = pl.BlockSpec(memory_space=pltpu.HBM)
    vmem = pl.BlockSpec(memory_space=pltpu.VMEM)
    out_types = [
        ((n_roll, tokens, q_width), low),
        ((n_roll, tokens, kv_width), low),
        ((n_roll, tokens, kv_width), low),
        ((rank, span), full),
        ((rank, span), full),
    ]
    outs = pl.pallas_call(
        partial(fused_kernel, n_seq, n_dp, n_roll, tokens, kv_heads, group, rank),
        out_shape=[vm(shape, kind) for shape, kind in out_types],
        in_specs=[anywhere] * 11,
        out_specs=[vmem] * len(out_types),
        scratch_shapes=[
            pltpu.SMEM((n_roll,), jnp.int32),
            pltpu.SMEM((n_roll,), jnp.int32),
            vm((2 * tokens, HEAD_WIDTH), full),
            vm((2 * tokens, HEAD_WIDTH), full),
            vm((n_roll, tokens, kv_width), low),
            vm((kv_heads, n_roll, 2, tokens, HEAD_WIDTH), low),
            vm((n_own, n_roll, 2, length, HEAD_WIDTH), low),
            vm((n_own, n_roll, 2, tokens, span), low),
            vm((n_own, n_roll, 2, tokens, span), low),
            vm((n_roll, tokens, q_width), low),
            vm((n_own, n_roll, tokens, span), low),
            vm((rank, q_width), low),
            vm((rank, q_width), low),
            vm((2, rank, n_roll * tokens), low),
            vm((n_roll, rank, 2 * tokens), low),
            vm((2, length, group * 2 * tokens), full),
            vm((length, group * 2 * tokens), low),
            vm((n_own, n_roll, 2, length, HEAD_WIDTH), low),
            vm((n_chips, kv_heads, n_roll, 2, tokens, HEAD_WIDTH), low),
            vm((n_own, n_roll, 2, tokens, span), low),
            vm((n_roll, rank, 2 * tokens), full),
            vm((n_roll, rank, 2 * tokens), full),
            vm((rank, span), full),
            vm((n_own, rank, span), low),
            vm((n_chips, rank, span), low),
            vm((n_own, rank, span), low),
            vm((n_chips, rank, span), low),
            vm((2, rank, span), low),
            vm((2, n_dp, rank, span // n_dp), low),
            vm((2, n_dp, rank, span // n_dp), low),
            vm((n_own, n_roll, 2, 2 * tokens, HEAD_WIDTH), low),
            vm((n_own, n_roll, 2, 2 * tokens, HEAD_WIDTH), low),
            dma((8,)),
            dma((kv_heads,)),
            dma((n_own, n_roll)),
            dma((n_own, n_roll)),
            dma((n_own, n_roll, 2, n_chips)),
            dma((n_own, n_roll, n_seq)),
            dma((n_own, n_roll)),
            dma((n_own, n_roll)),
            dma((n_own, n_roll)),
            dma((n_own, n_roll)),
            dma((n_own,)),
            dma((n_own,)),
            dma((2,)),
            dma((2,)),
            dma((n_own, n_roll, n_chips, 2)),
            dma((n_chips, kv_heads, n_roll)),
            dma((n_own, n_roll)),
            dma((n_own, n_roll)),
            dma((2, n_chips)),
            dma((2, n_chips)),
            dma((2, n_dp)),
            dma((2, n_dp)),
            dma((2, n_dp)),
            dma((2, n_dp)),
            dma((n_own, n_roll, 2)),
            dma((n_own, n_roll)),
            dma((n_own, n_roll)),
            dma((n_own, n_roll)),
            dma((n_own, n_roll)),
        ],
        compiler_params=pltpu.CompilerParams(
            collective_id=0, has_side_effects=True, vmem_limit_bytes=VMEM_LIMIT
        ),
    )(
        *[
            pltpu.with_memory_space_constraint(value, pltpu.HBM)
            for value in (
                offsets,
                lengths,
                jnp.asarray(cos_wide),
                jnp.asarray(sin_wide),
                queries,
                unrotated_key_rows,
                value_projection_rows,
                attention_output_gradient,
                normed_hidden_input,
                adapter_down_weight.T,
                adapter_up_weight,
            )
        ]
    )
    outs = pl.pallas_call(
        partial(write_kernel, len(out_types)),
        out_shape=[jax.ShapeDtypeStruct(shape, kind) for shape, kind in out_types],
        in_specs=[vmem] * len(out_types),
        out_specs=[anywhere] * len(out_types),
        scratch_shapes=[dma((len(out_types),))],
        compiler_params=pltpu.CompilerParams(vmem_limit_bytes=8 * 1024 * 1024),
    )(*outs)
    grad_query, grad_key, grad_value, grad_down, grad_up = outs
    return (grad_query, grad_key, grad_value, grad_down.T, grad_up)


def dispatch(mesh, *args):
    n_seq = mesh.shape["seq"]
    n_dp = mesh.shape["dp"]
    n_roll, tokens, q_width = args[0].shape
    kv_width = args[1].shape[2]
    kv_heads = kv_width // HEAD_WIDTH
    group = q_width // kv_width
    rows = 2 * tokens * group
    length = n_seq * tokens
    held = 3 * 2 * n_roll * length * kv_width + 10 * n_roll * tokens * q_width
    held = held + 12 * length * rows
    fits = held < VMEM_LIMIT // 2
    whole = kv_heads == n_seq and n_seq == 8 and 2 * tokens == HEAD_WIDTH
    whole = whole and 2 * tokens >= OFFSET_BOUND and (group * HEAD_WIDTH) % (n_dp * 128) == 0
    if not (fits and whole):
        return on_device(*args)
    return fused_on_device(n_seq, n_dp, *args)


def solution(mesh):
    in_specs = (
        P("dp", "seq", None),
        P("dp", "seq", None),
        P("dp", "seq", None),
        P("dp", "seq", None),
        P("dp", "seq", None),
        P(),
        P(),
        P("dp"),
        P("dp"),
    )
    out_specs = (
        P("dp", "seq", None),
        P("dp", "seq", None),
        P("dp", "seq", None),
        P("seq", None),
        P(None, "seq"),
    )
    return jax.shard_map(
        partial(dispatch, mesh), mesh=mesh, in_specs=in_specs, out_specs=out_specs, check_vma=False
    )
```

```python
from functools import partial

import math

import jax
import jax.numpy as jnp
import numpy as np
from jax import lax
from jax.experimental import pallas as pl
from jax.experimental.pallas import tpu as pltpu
from jax.sharding import PartitionSpec as P

HEAD_WIDTH = 128


rotary_base = 500000.0


def partner_2(value, axis, distance):
    mask = 2**distance
    pairs = [(source, source ^ mask) for source in range(lax.axis_size(axis))]
    return lax.ppermute(value, axis, pairs)


def rotary_tables(length, head_size):
    half_size = head_size // 2
    frequency = rotary_base ** (-(jnp.arange(half_size, dtype=jnp.float32) * 2.0 / head_size))
    angles = jnp.arange(length, dtype=jnp.float32)[:, None] * frequency[None, :]
    return (jnp.cos(angles), jnp.sin(angles))


def rotate(fields, cosine, sine_table, direction):
    half_size = fields.shape[-1] // 2
    first_half = fields[..., :half_size]
    second_half = fields[..., half_size:]
    cos_wide = cosine[:, None, :]
    sin_wide = direction * sine_table[:, None, :]
    return jnp.concatenate(
        [
            first_half * cos_wide - second_half * sin_wide,
            second_half * cos_wide + first_half * sin_wide,
        ],
        axis=-1,
    )


def contract_axes(first_operand, second_operand, first_axis, second_axis):
    return lax.dot_general(
        first_operand,
        second_operand,
        (((first_axis,), (second_axis,)), ((), ())),
        preferred_element_type=jnp.float32,
    )


def block_terms(rot_query, rot_key, value_head, grad_head, offset, begin_row, end_row, score_scale):
    row_index = jnp.arange(begin_row, end_row, dtype=jnp.int32)[:, None]
    col_index = jnp.arange(end_row, dtype=jnp.int32)[None, :]
    visible = (col_index == row_index) | (col_index >= offset) & (col_index <= row_index)
    query_block = rot_query[begin_row:end_row]
    grad_block = grad_head[begin_row:end_row]
    key_block = rot_key[:end_row]
    value_block = value_head[:end_row]
    scores = contract_axes(query_block, key_block, 1, 1) * score_scale
    row_max = jnp.max(jnp.where(visible, scores, -jnp.inf), axis=1, keepdims=True)
    row_total = jnp.sum(jnp.where(visible, jnp.exp(scores - row_max), 0.0), axis=1, keepdims=True)
    grad_prob = contract_axes(grad_block, value_block, 1, 1)
    probability = jnp.where(visible, jnp.exp(scores - row_max), 0.0) / row_total
    row_delta = jnp.sum(probability * grad_prob, axis=1, keepdims=True)
    prob_low = probability.astype(jnp.bfloat16)
    grad_score = (probability * (grad_prob - row_delta) * score_scale).astype(jnp.bfloat16)
    block_grad = jnp.dot(grad_score, key_block, preferred_element_type=jnp.float32)
    key_add = contract_axes(grad_score, query_block, 0, 0)
    value_add = contract_axes(prob_low, grad_block, 0, 0)
    return (block_grad, key_add, value_add)


def head_backward(rot_query, rot_key, value_head, grad_head, offset, block_rows):
    length = rot_query.shape[0]
    head_size = rot_query.shape[1]
    score_scale = head_size ** (-0.5)
    query_parts = []
    key_terms = []
    value_terms = []
    for block_index in range(length // block_rows):
        begin_row = block_index * block_rows
        end_row = begin_row + block_rows
        live_terms = partial(
            block_terms,
            rot_query,
            rot_key,
            value_head,
            grad_head,
            offset,
            begin_row,
            end_row,
            score_scale,
        )
        results = live_terms()
        block_grad, key_add, value_add = results
        query_parts.append(block_grad)
        key_terms.append(jnp.pad(key_add, ((0, length - end_row), (0, 0))))
        value_terms.append(jnp.pad(value_add, ((0, length - end_row), (0, 0))))
    key_accum = key_terms[0]
    value_accum = value_terms[0]
    for term_index in range(1, len(key_terms)):
        key_accum = key_accum + key_terms[term_index]
        value_accum = value_accum + value_terms[term_index]
    return (jnp.concatenate(query_parts, axis=0), key_accum, value_accum)


def arrange_rows(rows, share, part_rows, key_groups):
    rollout_count = rows.shape[0]
    split = rows.reshape(rollout_count, share, part_rows, key_groups, HEAD_WIDTH)
    return jnp.transpose(split, (0, 2, 3, 1, 4)).reshape(
        rollout_count, part_rows, key_groups * share, HEAD_WIDTH
    )


def join_group(paired, share, seq_parts, part_rows):
    my_index = lax.axis_index("seq")
    rollout_count = paired.shape[1]
    local_keys = paired.shape[3]
    joined = paired[None]
    for bit in range(share.bit_length() - 1):
        partner = partner_2(joined, "seq", bit)
        upper = my_index // (1 << bit) % 2
        joined = jnp.where(
            upper == 0,
            jnp.concatenate([joined, partner], axis=0),
            jnp.concatenate([partner, joined], axis=0),
        )
    ordered = joined.reshape(share, 2, rollout_count, seq_parts, part_rows, local_keys, HEAD_WIDTH)
    ordered = jnp.transpose(ordered, (1, 2, 3, 0, 4, 5, 6))
    return ordered.reshape(2, rollout_count, seq_parts * share * part_rows, local_keys, HEAD_WIDTH)


def reduce_group(partial_sums, share, seq_parts, part_rows):
    my_index = lax.axis_index("seq")
    rollout_count = partial_sums.shape[1]
    local_keys = partial_sums.shape[3]
    split = partial_sums.reshape(
        2, rollout_count, seq_parts, share, part_rows, local_keys, HEAD_WIDTH
    )
    split = jnp.transpose(split, (3, 0, 1, 2, 4, 5, 6))
    for bit in reversed(range(share.bit_length() - 1)):
        half = split.shape[0] // 2
        lower_half = split[:half]
        upper_half = split[half:]
        upper = my_index // (1 << bit) % 2
        keep = jnp.where(upper == 0, lower_half, upper_half)
        outgoing = jnp.where(upper == 0, upper_half, lower_half)
        split = keep + partner_2(outgoing.astype(jnp.bfloat16), "seq", bit).astype(outgoing.dtype)
    return split[0].reshape(2, rollout_count, seq_parts * part_rows, local_keys, HEAD_WIDTH)


def on_device(
    queries,
    unrotated_key_rows,
    value_projection_rows,
    attention_output_gradient,
    normed_hidden_input,
    adapter_down_weight,
    adapter_up_weight,
    lengths,
    offsets,
):
    rollout_count = queries.shape[0]
    tokens = queries.shape[1]
    seq_parts = lax.axis_size("seq")
    length = tokens * seq_parts
    query_width = queries.shape[2]
    head_count = query_width // HEAD_WIDTH
    key_groups = unrotated_key_rows.shape[2] // HEAD_WIDTH
    local_heads = head_count // seq_parts
    adapter_rank_size = adapter_down_weight.shape[1]
    share = max(1, seq_parts // key_groups)
    part_rows = tokens // share
    query_tokens = queries.reshape(rollout_count, tokens, head_count, HEAD_WIDTH)
    grad_tokens = attention_output_gradient.reshape(rollout_count, tokens, head_count, HEAD_WIDTH)
    key_arranged = arrange_rows(unrotated_key_rows, share, part_rows, key_groups)
    value_arranged = arrange_rows(value_projection_rows, share, part_rows, key_groups)
    query_heads, key_parted, value_parted, grad_heads = (
        lax.all_to_all(query_tokens, "seq", split_axis=2, concat_axis=1, tiled=True),
        lax.all_to_all(key_arranged, "seq", split_axis=2, concat_axis=1, tiled=True),
        lax.all_to_all(value_arranged, "seq", split_axis=2, concat_axis=1, tiled=True),
        lax.all_to_all(grad_tokens, "seq", split_axis=2, concat_axis=1, tiled=True),
    )
    paired = join_group(jnp.stack([key_parted, value_parted], axis=0), share, seq_parts, part_rows)
    key_heads = paired[0]
    value_heads = paired[1]
    local_keys = key_heads.shape[2]
    cosine, sine_table = rotary_tables(length, HEAD_WIDTH)
    positions = jnp.arange(length, dtype=jnp.int32)
    keep_mask = (positions[None, :] >= offsets[:, None]) & (positions[None, :] < lengths[:, None])
    grad_heads = jnp.where(keep_mask[:, :, None, None], grad_heads, jnp.zeros_like(grad_heads))
    rot_query = rotate(query_heads.astype(jnp.float32), cosine, sine_table, 1.0).astype(
        jnp.bfloat16
    )
    rot_key = rotate(key_heads.astype(jnp.float32), cosine, sine_table, 1.0).astype(jnp.bfloat16)
    block_rows = min(512, length)
    query_rolls = []
    key_rolls = []
    value_rolls = []
    for rollout_slot in range(rollout_count):
        query_list = []
        key_list = []
        value_list = []
        for head_slot in range(local_heads):
            key_slot = head_slot * local_keys // local_heads
            query_grad, key_grad, value_grad = head_backward(
                rot_query[rollout_slot, :, head_slot],
                rot_key[rollout_slot, :, key_slot],
                value_heads[rollout_slot, :, key_slot],
                grad_heads[rollout_slot, :, head_slot],
                offsets[rollout_slot],
                block_rows,
            )
            query_list.append(
                rotate(query_grad[:, None, :], cosine, sine_table, -1.0)[:, 0].astype(jnp.bfloat16)
            )
            key_list.append(
                rotate(key_grad[:, None, :], cosine, sine_table, -1.0)[:, 0].astype(jnp.bfloat16)
            )
            value_list.append(value_grad.astype(jnp.bfloat16))
        query_rolls.append(jnp.stack(query_list, axis=1))
        key_rolls.append(jnp.stack(key_list, axis=1))
        value_rolls.append(jnp.stack(value_list, axis=1))
    query_back = jnp.stack(query_rolls, axis=0)
    key_parts = jnp.stack(key_rolls, axis=0)
    value_parts = jnp.stack(value_rolls, axis=0)
    shared_heads = local_heads // local_keys
    key_local = (
        key_parts.astype(jnp.float32)
        .reshape(rollout_count, length, local_keys, shared_heads, HEAD_WIDTH)
        .sum(axis=3)
    )
    value_local = (
        value_parts.astype(jnp.float32)
        .reshape(rollout_count, length, local_keys, shared_heads, HEAD_WIDTH)
        .sum(axis=3)
    )
    summed = reduce_group(
        jnp.stack([key_local, value_local], axis=0), share, seq_parts, part_rows
    ).astype(jnp.bfloat16)
    query_result, key_result, value_result = (
        lax.all_to_all(query_back, "seq", split_axis=1, concat_axis=2, tiled=True),
        lax.all_to_all(summed[0], "seq", split_axis=1, concat_axis=2, tiled=True),
        lax.all_to_all(summed[1], "seq", split_axis=1, concat_axis=2, tiled=True),
    )
    key_total = jnp.transpose(
        key_result.reshape(rollout_count, part_rows, key_groups, share, HEAD_WIDTH), (0, 3, 1, 2, 4)
    ).reshape(rollout_count, tokens, key_groups * HEAD_WIDTH)
    value_total = jnp.transpose(
        value_result.reshape(rollout_count, part_rows, key_groups, share, HEAD_WIDTH),
        (0, 3, 1, 2, 4),
    ).reshape(rollout_count, tokens, key_groups * HEAD_WIDTH)
    flattened_query = query_result.reshape(rollout_count * tokens, query_width)
    hidden_state = normed_hidden_input.reshape(rollout_count * tokens, normed_hidden_input.shape[2])
    adapter_latent = jnp.dot(
        hidden_state, adapter_down_weight, preferred_element_type=jnp.float32
    ).astype(jnp.bfloat16)
    backward_gradient = contract_axes(flattened_query, adapter_up_weight, 1, 1).astype(jnp.bfloat16)
    joined_terms = lax.psum_scatter(
        jnp.concatenate(
            [
                contract_axes(hidden_state, backward_gradient, 0, 0),
                contract_axes(flattened_query, adapter_latent, 0, 0),
            ],
            axis=1,
        ).astype(jnp.bfloat16),
        "seq",
        scatter_dimension=0,
        tiled=True,
    ).astype(jnp.float32)
    down_local = joined_terms[:, :adapter_rank_size]
    up_local = joined_terms[:, adapter_rank_size:]
    down_sum, up_sum = (
        lax.psum(down_local.astype(jnp.bfloat16), "dp").astype(jnp.float32),
        lax.psum(up_local.astype(jnp.bfloat16), "dp").astype(jnp.float32),
    )
    return (
        flattened_query.reshape(rollout_count, tokens, query_width),
        key_total,
        value_total,
        down_sum,
        up_sum.T,
    )


VMEM_LIMIT = 48 * 1024 * 1024
MERGE_LAG = 3
HELD = 3
RELAYED = 5
SEND_AHEAD = 2
NEG = -1e30
OFFSET_BOUND = 32


def nt_dot(left, right):
    return lax.dot_general(
        left, right, (((1,), (1,)), ((), ())), preferred_element_type=jnp.float32
    )


def fused_kernel(
    n_seq,
    n_dp,
    n_roll,
    tokens,
    kv_heads,
    group,
    rank,
    off_hbm,
    len_hbm,
    cos_hbm,
    sin_hbm,
    q_hbm,
    k_hbm,
    v_hbm,
    g_hbm,
    hid_hbm,
    down_hbm,
    up_hbm,
    gq_ref,
    gk_ref,
    gv_ref,
    gd_ref,
    gu_ref,
    off_ref,
    len_ref,
    cos_ref,
    sin_ref,
    k_raw,
    kv_own,
    kv_all,
    q_all,
    g_all,
    hid_own,
    hid_other,
    down_ref,
    up_ref,
    lat_all,
    lat_roll,
    score_buf,
    prob_buf,
    dkv_own,
    dkv_all,
    gq_all,
    back_acc,
    back_got,
    up_acc,
    up_own,
    up_got,
    dn_own,
    dn_got,
    z_own,
    z_got,
    z_all,
    merge_buf,
    relay_buf,
    loc_sem,
    v_sem,
    ql_sem,
    gl_sem,
    kv_send,
    kv_recv,
    q_send,
    q_recv,
    g_send,
    g_recv,
    hid_send,
    hid_recv,
    one_send,
    one_recv,
    dk_send,
    dk_recv,
    gq_send,
    gq_recv,
    ad_send,
    ad_recv,
    rs_send,
    rs_recv,
    ag_send,
    ag_recv,
    fw_send,
    mg_send,
    mg_recv,
    rl_send,
    rl_recv,
):
    me = lax.axis_index("seq")
    my_dp = lax.axis_index("dp")
    chip = me // 2
    core = me % 2
    partner = me + 1 - 2 * core
    n_chips = n_seq // 2
    n_own = kv_heads // 2
    width = HEAD_WIDTH
    half = width // 2
    span = group * width
    chip_tokens = 2 * tokens
    rows = group * chip_tokens
    scale = width ** (-0.5)
    exp_scale = scale * math.log2(math.e)
    piece = span // n_dp
    n_units = n_own * n_roll

    def lanes(index, size):
        return pl.ds(pl.multiple_of(index * size, size), size)

    def seq_rows(device):
        return pl.ds(pl.multiple_of(device * tokens, tokens), tokens)

    def local(src, dst, sem):
        return pltpu.make_async_copy(src, dst, sem)

    def remote(src, dst, send, recv, where):
        return pltpu.make_async_remote_copy(
            src_ref=src, dst_ref=dst, send_sem=send, recv_sem=recv, device_id=where
        )

    def each_unit(body):
        def step(index, carry):
            body(index // n_roll, index % n_roll)
            return carry

        lax.fori_loop(0, n_own * n_roll, step, 0)

    barrier = pltpu.get_barrier_semaphore()
    for step in range(1, n_seq):
        pl.semaphore_signal(barrier, inc=1, device_id={"seq": lax.rem(me + step, n_seq)})
    for step in range(1, n_dp):
        pl.semaphore_signal(barrier, inc=1, device_id={"dp": lax.rem(my_dp + step, n_dp)})

    chip_rows = pl.ds(pl.multiple_of(chip * chip_tokens, chip_tokens), chip_tokens)
    k_load = local(k_hbm, k_raw, loc_sem.at[0])
    cos_load = local(cos_hbm.at[chip_rows], cos_ref, loc_sem.at[1])
    sin_load = local(sin_hbm.at[chip_rows], sin_ref, loc_sem.at[2])
    off_load = local(off_hbm, off_ref, loc_sem.at[3])
    len_load = local(len_hbm, len_ref, loc_sem.at[4])
    hid_load = local(hid_hbm, hid_own, loc_sem.at[5])
    down_load = local(down_hbm, down_ref, loc_sem.at[6])
    up_load = local(up_hbm, up_ref, loc_sem.at[7])

    def v_load(h):
        return local(v_hbm.at[:, :, lanes(h, width)], kv_own.at[h, :, 1], v_sem.at[h])

    def q_load(i, r):
        h = 2 * i + core
        return local(q_hbm.at[r, :, lanes(h, span)], q_all.at[i, r, core], ql_sem.at[i, r])

    def g_load(i, r):
        h = 2 * i + core
        return local(g_hbm.at[r, :, lanes(h, span)], g_all.at[i, r, core], gl_sem.at[i, r])

    def load_queries(i, r):
        q_load(i, r).start()
        g_load(i, r).start()

    k_load.start()
    cos_load.start()
    sin_load.start()
    for h in range(kv_heads):
        v_load(h).start()
    off_load.start()
    len_load.start()
    each_unit(load_queries)
    hid_load.start()
    down_load.start()
    up_load.start()

    def q_copy(i, r):
        h = 2 * i + 1 - core
        return remote(
            q_hbm.at[r, :, lanes(h, span)],
            q_all.at[i, r, core],
            q_send.at[i, r],
            q_recv.at[i, r],
            {"seq": partner},
        )

    def g_copy(i, r):
        h = 2 * i + 1 - core
        return remote(
            g_hbm.at[r, :, lanes(h, span)],
            g_all.at[i, r, core],
            g_send.at[i, r],
            g_recv.at[i, r],
            {"seq": partner},
        )

    def hid_copy(i):
        h = 2 * i + 1 - core
        return remote(
            hid_hbm.at[:, :, lanes(h, span)],
            hid_other.at[i],
            hid_send.at[i],
            hid_recv.at[i],
            {"seq": partner},
        )

    def send_queries(i, r):
        q_copy(i, r).start()
        g_copy(i, r).start()

    def gather_copy(i, r, parity, chip_step):
        h = 2 * i + parity
        return remote(
            kv_own.at[h, r],
            kv_all.at[i, r, :, seq_rows(me), :],
            kv_send.at[i, r, parity, chip_step],
            kv_recv.at[i, r, me],
            {"seq": 2 * (chip + chip_step) + parity},
        )

    def pair_copy(i, r):
        h = 2 * i + 1 - core
        return remote(
            kv_own.at[h, r],
            kv_all.at[i, r, :, seq_rows(me), :],
            kv_send.at[i, r, 0, 0],
            kv_recv.at[i, r, me],
            {"seq": partner},
        )

    n_passed = n_own // 2

    def gather_ops(i, r, act, later=False):
        if not later:
            act(pair_copy(i, r))
        for chip_step in range(1, n_chips):
            mine = chip + chip_step < n_chips
            if chip_step == 3:
                mine = mine & (i >= n_passed)
            if chip_step == 1:
                mine = mine & ((chip == 1) if later else (chip != 1))
            elif later:
                continue

            @pl.when(mine)
            def _():
                for parity in range(2):
                    act(gather_copy(i, r, parity, chip_step))

    def later_ops(index, act):
        @pl.when((chip == 1) & (index >= n_passed * n_roll) & (index < n_units))
        def _():
            gather_ops(index // n_roll, index % n_roll, act, later=True)

    def gather_got(i, r, device):
        return remote(
            kv_own.at[0, r],
            kv_all.at[i, r, :, seq_rows(device), :],
            kv_send.at[i, r, 0, 0],
            kv_recv.at[i, r, device],
            {"seq": partner},
        )

    def pass_copy(i, r, source_core):
        source = 2 * (chip - 2) + source_core
        return remote(
            kv_all.at[i, r, :, seq_rows(source), :],
            kv_all.at[i, r, :, seq_rows(source), :],
            fw_send.at[i, r, source_core],
            kv_recv.at[i, r, source],
            {"seq": 2 * (5 - chip) + core},
        )

    def pass_on(index, carry):
        i = index // n_roll
        r = index % n_roll
        gather_ops(i, r, lambda copy: copy.start())

        @pl.when(i < n_passed)
        def _():
            for source_core in range(2):
                gather_got(i, r, 2 * (chip - 2) + source_core).wait_recv()
                pass_copy(i, r, source_core).start()

        return carry

    def passed_sent(i, r):
        @pl.when((chip >= 2) & (i < n_passed))
        def _():
            for source_core in range(2):
                pass_copy(i, r, source_core).wait_send()

    def gather_wait(i, r):
        def block(source):
            for source_core in range(2):
                gather_got(i, r, 2 * source + source_core).wait_recv()

        gather_got(i, r, partner).wait_recv()

        @pl.when((chip == 1) | ((chip >= 2) & (i >= n_passed)))
        def _():
            block(0)

        @pl.when((chip >= 2) & (i >= n_passed))
        def _():
            block(1)

        @pl.when((chip == 2) & (i < n_passed))
        def _():
            block(1)

        @pl.when((chip == 3) & (i < n_passed))
        def _():
            block(0)

        @pl.when(chip == 3)
        def _():
            block(2)

    def reduce_copy(i, r, target_chip, target_core):
        target = 2 * target_chip + target_core
        return remote(
            dkv_own.at[i, r, :, seq_rows(target), :],
            dkv_all.at[chip, 2 * i + core, r],
            dk_send.at[i, r, target_chip, target_core],
            dk_recv.at[chip, 2 * i + core, r],
            {"seq": target},
        )

    def chip_block(target_chip):
        return pl.ds(target_chip * chip_tokens, chip_tokens)

    def merge_copy(i, r, target_chip):
        return remote(
            dkv_own.at[i, r, :, chip_block(0), :],
            merge_buf.at[i, r],
            mg_send.at[i, r],
            mg_recv.at[i, r],
            {"seq": 2 * target_chip + core},
        )

    def relay_copy(i, r):
        return remote(
            dkv_own.at[i, r, :, chip_block(1), :],
            relay_buf.at[i, r],
            rl_send.at[i, r],
            rl_recv.at[i, r],
            {"seq": core},
        )

    def pass_back_copy(i, r, target_core):
        return remote(
            relay_buf.at[i, r, :, pl.ds(target_core * tokens, tokens), :],
            dkv_all.at[2, 2 * i + core, r],
            dk_send.at[i, r, 1, target_core],
            dk_recv.at[2, 2 * i + core, r],
            {"seq": 2 + target_core},
        )

    def merges(r):
        return ((chip == 1) & (r % 2 == 0)) | ((chip == 2) & (r % 2 == 1))

    def block_ops(i, r, target_chip, act):
        for target_core in range(2):
            act(reduce_copy(i, r, target_chip, target_core))

    def reduce_ops(i, r, act):
        act(reduce_copy(i, r, chip, 1 - core))
        index = i * n_roll + r

        @pl.when(((chip == 1) | (chip == 2)) & ~merges(r))
        def _():
            block_ops(i, r, 0, act)

        @pl.when((chip == 2) & (index < RELAYED))
        def _():
            act(relay_copy(i, r))

        @pl.when((chip == 3) & (index < n_units - HELD))
        def _():
            top_ops(i, r, act)

    def to_merge_ops(i, r, act):
        act(merge_copy(i, r, 1 + r % 2))

    def top_ops(i, r, act):
        to_merge_ops(i, r, act)
        block_ops(i, r, 2, act)
        block_ops(i, r, 1, act)

    def held_ops(act):
        @pl.when(chip == 2)
        def _():
            for index in range(RELAYED, n_units):
                block_ops(*divmod(index, n_roll), 1, act)

        @pl.when(chip == 3)
        def _():
            held = [divmod(index, n_roll) for index in range(n_units - HELD, n_units)]
            for i, r in held:
                to_merge_ops(i, r, act)
            for i, r in held:
                block_ops(i, r, 1, act)
                block_ops(i, r, 2, act)

    def merge(i, r):
        @pl.when(merges(r))
        def _():
            merge_copy(i, r, 0).wait_recv()
            for t in range(2):
                block = dkv_own[i, r, t, :chip_tokens, :].astype(jnp.float32)
                block = block + merge_buf[i, r, t].astype(jnp.float32)
                dkv_own[i, r, t, :chip_tokens, :] = block.astype(jnp.bfloat16)
            block_ops(i, r, 0, lambda copy: copy.start())

    def pass_back(i, r):
        relay_copy(i, r).wait_recv()
        for target_core in range(2):
            pass_back_copy(i, r, target_core).start()

    def reduce_got(source, h, r):
        return remote(
            dkv_own.at[0, 0, :, pl.ds(0, tokens), :],
            dkv_all.at[source, h, r],
            dk_send.at[0, 0, 0, 0],
            dk_recv.at[source, h, r],
            {"seq": partner},
        )

    def gq_copy(i, r, parity):
        return remote(
            gq_all.at[i, r, 1 - core],
            gq_ref.at[r, :, lanes(2 * i + parity, span)],
            gq_send.at[i, r],
            gq_recv.at[i, r],
            {"seq": partner},
        )

    def adapter_copy(t, own, got, source, target_chip):
        return remote(
            own.at[target_chip],
            got.at[source],
            ad_send.at[t, target_chip],
            ad_recv.at[t, source],
            {"seq": 2 * target_chip + core},
        )

    k_load.wait()
    cos_load.wait()
    sin_load.wait()
    own_rows = pl.ds(pl.multiple_of(core * tokens, tokens), tokens)
    cos_own = cos_ref[own_rows, :]
    sin_own = sin_ref[own_rows, :]
    for h in range(kv_heads):
        for r in range(n_roll):
            key = k_raw[r, :, h * width : (h + 1) * width].astype(jnp.float32)
            key = key * cos_own + pltpu.roll(key, half, 1) * sin_own
            kv_own[h, r, 0] = key.astype(jnp.bfloat16)
    for h in range(kv_heads):
        v_load(h).wait()
    for i in range(n_own):
        for r in range(n_roll):
            kv_all[i, r, :, seq_rows(me), :] = kv_own[2 * i + core, r]

    pl.semaphore_wait(barrier, n_seq + n_dp - 2)

    @pl.when(chip < 2)
    def _():
        each_unit(lambda i, r: gather_ops(i, r, lambda copy: copy.start()))

    each_unit(send_queries)

    hid_load.wait()
    down_load.wait()
    flat = n_roll * tokens
    hid_rows = hid_own[...].reshape(flat, hid_own.shape[2])
    lat_all[core] = nt_dot(down_ref[...], hid_rows).astype(jnp.bfloat16)
    lat_copy = remote(
        lat_all.at[core], lat_all.at[core], one_send.at[0], one_recv.at[0], {"seq": partner}
    )
    lat_copy.start()
    for i in range(n_own):
        hid_copy(i).start()

    @pl.when(chip >= 2)
    def _():
        lax.fori_loop(0, n_units, pass_on, 0)

    back_acc[...] = jnp.zeros_like(back_acc)
    up_acc[...] = jnp.zeros_like(up_acc)
    up_load.wait()
    off_load.wait()
    len_load.wait()
    remote(
        lat_all.at[core], lat_all.at[1 - core], one_send.at[0], one_recv.at[0], {"seq": partner}
    ).wait_recv()
    for r in range(n_roll):
        lane = slice(r * tokens, (r + 1) * tokens)
        lat_roll[r] = jnp.concatenate([lat_all[0, :, lane], lat_all[1, :, lane]], axis=1)

    def attend(i, r, blocks):
        n_keys = blocks * chip_tokens
        offset = off_ref[r]
        position = chip * chip_tokens + lax.broadcasted_iota(jnp.int32, (chip_tokens, width), 0)
        keep = (position >= offset) & (position < len_ref[r])
        cos = cos_ref[...]
        sin = sin_ref[...]
        queries = []
        grads = []
        for j in range(group):
            lane = slice(j * width, (j + 1) * width)
            query = q_all[i, r, :, :, lane].reshape(chip_tokens, width).astype(jnp.float32)
            query = query * cos + pltpu.roll(query, half, 1) * sin
            queries.append(query.astype(jnp.bfloat16))
            grad = g_all[i, r, :, :, lane].reshape(chip_tokens, width).astype(jnp.float32)
            grads.append(jnp.where(keep, grad, 0.0).astype(jnp.bfloat16))
        query = jnp.concatenate(queries, axis=0)
        grad = jnp.concatenate(grads, axis=0)
        key = kv_all[i, r, 0, :n_keys, :]

        row_max = None
        for b in range(blocks):
            keys = slice(b * chip_tokens, (b + 1) * chip_tokens)
            score = nt_dot(kv_all[i, r, 0, keys, :], query)
            if b == blocks - 1 or b * chip_tokens < OFFSET_BOUND:
                key_row = lax.broadcasted_iota(jnp.int32, (chip_tokens, rows), 0)
                visible = key_row + b * chip_tokens >= offset
                if b == blocks - 1:
                    query_row = lax.broadcasted_iota(jnp.int32, (chip_tokens, rows), 1) % chip_tokens
                    visible = (key_row == query_row) | (visible & (key_row <= query_row))
                score = jnp.where(visible, score, NEG)
            score_buf[0, keys, :] = score
            part = jnp.max(score, axis=0, keepdims=True)
            row_max = part if row_max is None else jnp.maximum(row_max, part)
        total = None
        delta = None
        for b in range(blocks):
            keys = slice(b * chip_tokens, (b + 1) * chip_tokens)
            weight = jnp.exp2((score_buf[0, keys, :] - row_max) * exp_scale)
            grad_prob = nt_dot(kv_all[i, r, 1, keys, :], grad)
            score_buf[0, keys, :] = weight
            score_buf[1, keys, :] = grad_prob
            part = jnp.sum(weight, axis=0, keepdims=True)
            total = part if total is None else total + part
            part = jnp.sum(weight * grad_prob, axis=0, keepdims=True)
            delta = part if delta is None else delta + part
        inverse = 1.0 / total
        delta = delta * inverse
        inverse_scaled = inverse * scale
        for b in range(blocks):
            keys = slice(b * chip_tokens, (b + 1) * chip_tokens)
            weight = score_buf[0, keys, :]
            prob = (weight * inverse).astype(jnp.bfloat16)
            slope = ((weight * inverse_scaled) * (score_buf[1, keys, :] - delta)).astype(jnp.bfloat16)
            prob_buf[keys, :] = slope
            dkv_own[i, r, 1, keys, :] = jnp.dot(
                prob, grad, preferred_element_type=jnp.float32
            ).astype(jnp.bfloat16)
            dkv_own[i, r, 0, keys, :] = jnp.dot(
                slope, query, preferred_element_type=jnp.float32
            ).astype(jnp.bfloat16)
        back = jnp.dot(key.T, prob_buf[:n_keys, :], preferred_element_type=jnp.float32).T
        for j in range(group):
            part = back[j * chip_tokens : (j + 1) * chip_tokens]
            part = part * cos - pltpu.roll(part, half, 1) * sin
            part = part.astype(jnp.bfloat16).reshape(2, tokens, width)
            gq_all[i, r, :, :, j * width : (j + 1) * width] = part

    def unit(i, r):
        h = 2 * i + core
        gather_wait(i, r)
        later_ops(i * n_roll + r + SEND_AHEAD, lambda copy: copy.start())
        q_load(i, r).wait()
        g_load(i, r).wait()
        remote(
            q_hbm.at[r, :, lanes(h, span)],
            q_all.at[i, r, 1 - core],
            q_send.at[i, r],
            q_recv.at[i, r],
            {"seq": partner},
        ).wait_recv()
        remote(
            g_hbm.at[r, :, lanes(h, span)],
            g_all.at[i, r, 1 - core],
            g_send.at[i, r],
            g_recv.at[i, r],
            {"seq": partner},
        ).wait_recv()
        for blocks in range(1, n_chips + 1):

            @pl.when(chip == blocks - 1)
            def _():
                attend(i, r, blocks)

        reduce_ops(i, r, lambda copy: copy.start())
        gq_copy(i, r, core).start()
        late = i * n_roll + r - MERGE_LAG

        @pl.when(late >= 0)
        def _():
            merge(late // n_roll, late % n_roll)

        dkv_all[chip, h, r] = dkv_own[i, r, :, seq_rows(me), :]
        gq_ref[r, :, lanes(h, span)] = gq_all[i, r, core]
        grad_query = gq_all[i, r].reshape(chip_tokens, span)
        back_acc[r] = back_acc[r] + nt_dot(up_ref[:, lanes(h, span)], grad_query)
        up_part = jnp.dot(lat_roll[r], grad_query, preferred_element_type=jnp.float32)
        up_total = jnp.where(r == 0, 0.0, up_acc[...]) + up_part
        up_acc[...] = up_total

        @pl.when(r == n_roll - 1)
        def _():
            up_own[i] = up_total.astype(jnp.bfloat16)

            @pl.when(i != chip)
            def _():
                adapter_copy(1, up_own, up_got, chip, i).start()

    each_unit(unit)

    back_copy = remote(back_acc, back_got, one_send.at[1], one_recv.at[1], {"seq": partner})
    back_copy.start()
    for i in range(n_own):
        hid_copy(i).wait_recv()
    back_copy.wait_recv()
    sums = [(back_acc[r] + back_got[r]).astype(jnp.bfloat16) for r in range(n_roll)]
    first = jnp.concatenate([part[:, :tokens] for part in sums], axis=1)
    second = jnp.concatenate([part[:, tokens:] for part in sums], axis=1)
    back_own = jnp.where(core == 0, first, second)
    back_other = jnp.where(core == 0, second, first)
    for i in range(n_own):
        own = hid_own[:, :, lanes(2 * i + core, span)].reshape(flat, span)
        other = hid_other[i].reshape(flat, span)
        dn_own[i] = (
            jnp.dot(back_own, own, preferred_element_type=jnp.float32)
            + jnp.dot(back_other, other, preferred_element_type=jnp.float32)
        ).astype(jnp.bfloat16)

        @pl.when(i != chip)
        def _():
            adapter_copy(0, dn_own, dn_got, chip, i).start()

    def owner_sum(t, own, got):
        total = own[chip].astype(jnp.float32)
        for step in range(1, n_chips):
            source = lax.rem(chip + step, n_chips)
            adapter_copy(t, own, got, source, 0).wait_recv()
            total = total + got[source].astype(jnp.float32)
        z_own[t] = total.astype(jnp.bfloat16)

    def scatter_copy(t, target):
        return remote(
            z_own.at[t, :, lanes(target, piece)],
            z_got.at[t, my_dp],
            rs_send.at[t, target],
            rs_recv.at[t, my_dp],
            {"dp": target},
        )

    def scatter_start(t):
        for step in range(1, n_dp):
            scatter_copy(t, lax.rem(my_dp + step, n_dp)).start()

    def collect_copy(t, target):
        return remote(
            z_all.at[t, my_dp],
            z_all.at[t, my_dp],
            ag_send.at[t, target],
            ag_recv.at[t, my_dp],
            {"dp": target},
        )

    def collect_start(t):
        total = z_own[t, :, lanes(my_dp, piece)].astype(jnp.float32)
        for step in range(1, n_dp):
            source = lax.rem(my_dp + step, n_dp)
            remote(
                z_own.at[t, :, lanes(source, piece)],
                z_got.at[t, source],
                rs_send.at[t, source],
                rs_recv.at[t, source],
                {"dp": source},
            ).wait_recv()
            total = total + z_got[t, source].astype(jnp.float32)
        z_all[t, my_dp] = total.astype(jnp.bfloat16)
        for step in range(1, n_dp):
            collect_copy(t, lax.rem(my_dp + step, n_dp)).start()

    def collect_out(t, out):
        for step in range(1, n_dp):
            source = lax.rem(my_dp + step, n_dp)
            remote(
                z_all.at[t, source],
                z_all.at[t, source],
                ag_send.at[t, source],
                ag_recv.at[t, source],
                {"dp": source},
            ).wait_recv()
        for d in range(n_dp):
            out[:, d * piece : (d + 1) * piece] = z_all[t, d].astype(jnp.float32)

    held_ops(lambda copy: copy.start())

    @pl.when(chip == 0)
    def _():
        for index in range(RELAYED):
            pass_back(*divmod(index, n_roll))

    owner_sum(1, up_own, up_got)
    scatter_start(1)

    cos_own = cos_ref[own_rows, :]
    sin_own = sin_ref[own_rows, :]

    n_sources = jnp.where(chip == 0, n_chips - 1, n_chips)

    def finish(h, r):
        @pl.when(h % 2 != core)
        def _():
            reduce_got(chip, h, r).wait_recv()

        for source in range(1, n_chips):

            @pl.when((source > chip) & (source < n_sources))
            def _():
                reduce_got(source, h, r).wait_recv()

        def add(source, totals):
            return tuple(
                totals[t] + dkv_all[source, h, r, t].astype(jnp.float32) for t in range(2)
            )

        first = tuple(dkv_all[chip, h, r, t].astype(jnp.float32) for t in range(2))
        key, value = lax.fori_loop(chip + 1, n_sources, add, first)
        key = key * cos_own - pltpu.roll(key, half, 1) * sin_own
        gk_ref[r, :, lanes(h, width)] = key.astype(jnp.bfloat16)
        gv_ref[r, :, lanes(h, width)] = value.astype(jnp.bfloat16)

    def finish_step(index, carry):
        finish(index // n_roll, index % n_roll)
        return carry

    early = (kv_heads - 4) * n_roll
    lax.fori_loop(0, early, finish_step, 0)
    collect_start(1)
    owner_sum(0, dn_own, dn_got)
    scatter_start(0)

    def merge_step(index, carry):
        merge(index // n_roll, index % n_roll)
        return carry

    lax.fori_loop(max(0, n_units - MERGE_LAG), n_units, merge_step, 0)

    collect_out(1, gu_ref)
    each_unit(lambda i, r: gq_copy(i, r, 1 - core).wait_recv())
    collect_start(0)


    lax.fori_loop(early, kv_heads * n_roll, finish_step, 0)

    each_unit(lambda i, r: gather_ops(i, r, lambda copy: copy.wait_send()))
    each_unit(lambda i, r: later_ops(i * n_roll + r, lambda copy: copy.wait_send()))
    each_unit(lambda i, r: reduce_ops(i, r, lambda copy: copy.wait_send()))
    held_ops(lambda copy: copy.wait_send())
    each_unit(passed_sent)

    def merged_sent(i, r):
        @pl.when(merges(r))
        def _():
            block_ops(i, r, 0, lambda copy: copy.wait_send())

        @pl.when((chip == 0) & (i * n_roll + r < RELAYED))
        def _():
            for target_core in range(2):
                pass_back_copy(i, r, target_core).wait_send()

    each_unit(merged_sent)

    def sent(i, r):
        q_copy(i, r).wait_send()
        g_copy(i, r).wait_send()
        gq_copy(i, r, core).wait_send()

    each_unit(sent)
    lat_copy.wait_send()
    back_copy.wait_send()
    for i in range(n_own):
        hid_copy(i).wait_send()

        @pl.when(i != chip)
        def _():
            adapter_copy(0, dn_own, dn_got, chip, i).wait_send()
            adapter_copy(1, up_own, up_got, chip, i).wait_send()

    collect_out(0, gd_ref)
    for t in range(2):
        for step in range(1, n_dp):
            target = lax.rem(my_dp + step, n_dp)
            scatter_copy(t, target).wait_send()
            collect_copy(t, target).wait_send()


def write_kernel(n_outs, *refs):
    sem = refs[2 * n_outs]
    copies = [
        pltpu.make_async_copy(refs[n], refs[n_outs + n], sem.at[n]) for n in range(n_outs)
    ]
    for copy in copies:
        copy.start()
    for copy in copies:
        copy.wait()


def fused_on_device(
    n_seq,
    n_dp,
    queries,
    unrotated_key_rows,
    value_projection_rows,
    attention_output_gradient,
    normed_hidden_input,
    adapter_down_weight,
    adapter_up_weight,
    lengths,
    offsets,
):
    n_roll, tokens, q_width = queries.shape
    kv_width = unrotated_key_rows.shape[2]
    kv_heads = kv_width // HEAD_WIDTH
    group = q_width // kv_width
    rank = adapter_down_weight.shape[1]
    length = n_seq * tokens
    n_chips = n_seq // 2
    n_own = kv_heads // 2
    half = HEAD_WIDTH // 2
    frequency = rotary_base ** (-(np.arange(half, dtype=np.float32) * 2.0 / HEAD_WIDTH))
    angles = np.arange(length, dtype=np.float32)[:, None] * frequency.astype(np.float32)[None, :]
    cosine, sine = np.cos(angles), np.sin(angles)
    cos_wide = np.concatenate([cosine, cosine], axis=1).astype(np.float32)
    sin_wide = np.concatenate([-sine, sine], axis=1).astype(np.float32)
    span = q_width // n_seq
    low = jnp.bfloat16
    full = jnp.float32
    dma = pltpu.SemaphoreType.DMA
    vm = pltpu.VMEM
    anywhere = pl.BlockSpec(memory_space=pltpu.HBM)
    vmem = pl.BlockSpec(memory_space=pltpu.VMEM)
    out_types = [
        ((n_roll, tokens, q_width), low),
        ((n_roll, tokens, kv_width), low),
        ((n_roll, tokens, kv_width), low),
        ((rank, span), full),
        ((rank, span), full),
    ]
    outs = pl.pallas_call(
        partial(fused_kernel, n_seq, n_dp, n_roll, tokens, kv_heads, group, rank),
        out_shape=[vm(shape, kind) for shape, kind in out_types],
        in_specs=[anywhere] * 11,
        out_specs=[vmem] * len(out_types),
        scratch_shapes=[
            pltpu.SMEM((n_roll,), jnp.int32),
            pltpu.SMEM((n_roll,), jnp.int32),
            vm((2 * tokens, HEAD_WIDTH), full),
            vm((2 * tokens, HEAD_WIDTH), full),
            vm((n_roll, tokens, kv_width), low),
            vm((kv_heads, n_roll, 2, tokens, HEAD_WIDTH), low),
            vm((n_own, n_roll, 2, length, HEAD_WIDTH), low),
            vm((n_own, n_roll, 2, tokens, span), low),
            vm((n_own, n_roll, 2, tokens, span), low),
            vm((n_roll, tokens, q_width), low),
            vm((n_own, n_roll, tokens, span), low),
            vm((rank, q_width), low),
            vm((rank, q_width), low),
            vm((2, rank, n_roll * tokens), low),
            vm((n_roll, rank, 2 * tokens), low),
            vm((2, length, group * 2 * tokens), full),
            vm((length, group * 2 * tokens), low),
            vm((n_own, n_roll, 2, length, HEAD_WIDTH), low),
            vm((n_chips, kv_heads, n_roll, 2, tokens, HEAD_WIDTH), low),
            vm((n_own, n_roll, 2, tokens, span), low),
            vm((n_roll, rank, 2 * tokens), full),
            vm((n_roll, rank, 2 * tokens), full),
            vm((rank, span), full),
            vm((n_own, rank, span), low),
            vm((n_chips, rank, span), low),
            vm((n_own, rank, span), low),
            vm((n_chips, rank, span), low),
            vm((2, rank, span), low),
            vm((2, n_dp, rank, span // n_dp), low),
            vm((2, n_dp, rank, span // n_dp), low),
            vm((n_own, n_roll, 2, 2 * tokens, HEAD_WIDTH), low),
            vm((n_own, n_roll, 2, 2 * tokens, HEAD_WIDTH), low),
            dma((8,)),
            dma((kv_heads,)),
            dma((n_own, n_roll)),
            dma((n_own, n_roll)),
            dma((n_own, n_roll, 2, n_chips)),
            dma((n_own, n_roll, n_seq)),
            dma((n_own, n_roll)),
            dma((n_own, n_roll)),
            dma((n_own, n_roll)),
            dma((n_own, n_roll)),
            dma((n_own,)),
            dma((n_own,)),
            dma((2,)),
            dma((2,)),
            dma((n_own, n_roll, n_chips, 2)),
            dma((n_chips, kv_heads, n_roll)),
            dma((n_own, n_roll)),
            dma((n_own, n_roll)),
            dma((2, n_chips)),
            dma((2, n_chips)),
            dma((2, n_dp)),
            dma((2, n_dp)),
            dma((2, n_dp)),
            dma((2, n_dp)),
            dma((n_own, n_roll, 2)),
            dma((n_own, n_roll)),
            dma((n_own, n_roll)),
            dma((n_own, n_roll)),
            dma((n_own, n_roll)),
        ],
        compiler_params=pltpu.CompilerParams(
            collective_id=0, has_side_effects=True, vmem_limit_bytes=VMEM_LIMIT
        ),
    )(
        *[
            pltpu.with_memory_space_constraint(value, pltpu.HBM)
            for value in (
                offsets,
                lengths,
                jnp.asarray(cos_wide),
                jnp.asarray(sin_wide),
                queries,
                unrotated_key_rows,
                value_projection_rows,
                attention_output_gradient,
                normed_hidden_input,
                adapter_down_weight.T,
                adapter_up_weight,
            )
        ]
    )
    outs = pl.pallas_call(
        partial(write_kernel, len(out_types)),
        out_shape=[jax.ShapeDtypeStruct(shape, kind) for shape, kind in out_types],
        in_specs=[vmem] * len(out_types),
        out_specs=[anywhere] * len(out_types),
        scratch_shapes=[dma((len(out_types),))],
        compiler_params=pltpu.CompilerParams(vmem_limit_bytes=8 * 1024 * 1024),
    )(*outs)
    grad_query, grad_key, grad_value, grad_down, grad_up = outs
    return (grad_query, grad_key, grad_value, grad_down.T, grad_up)


def dispatch(mesh, *args):
    n_seq = mesh.shape["seq"]
    n_dp = mesh.shape["dp"]
    n_roll, tokens, q_width = args[0].shape
    kv_width = args[1].shape[2]
    kv_heads = kv_width // HEAD_WIDTH
    group = q_width // kv_width
    rows = 2 * tokens * group
    length = n_seq * tokens
    held = 3 * 2 * n_roll * length * kv_width + 10 * n_roll * tokens * q_width
    held = held + 12 * length * rows
    fits = held < VMEM_LIMIT // 2
    whole = kv_heads == n_seq and n_seq == 8 and 2 * tokens == HEAD_WIDTH
    whole = whole and 2 * tokens >= OFFSET_BOUND and (group * HEAD_WIDTH) % (n_dp * 128) == 0
    if not (fits and whole):
        return on_device(*args)
    return fused_on_device(n_seq, n_dp, *args)


def solution(mesh):
    in_specs = (
        P("dp", "seq", None),
        P("dp", "seq", None),
        P("dp", "seq", None),
        P("dp", "seq", None),
        P("dp", "seq", None),
        P(),
        P(),
        P("dp"),
        P("dp"),
    )
    out_specs = (
        P("dp", "seq", None),
        P("dp", "seq", None),
        P("dp", "seq", None),
        P("seq", None),
        P(None, "seq"),
    )
    return jax.shard_map(
        partial(dispatch, mesh), mesh=mesh, in_specs=in_specs, out_specs=out_specs, check_vma=False
    )
```
